32 devices in a mesh: leaf: 32 (over z, y, x, core).
Axes of the slice: x: 2, y: 2, z: 4, core: 2. Of those that a mesh axis runs over, the one named last changes fastest.
Arguments:
- shots: float32 [32768, 2048], P('leaf'), may hold values from -6 to 6
- leaf_inverse: float32 [32768, 1024], P('leaf'), may hold values from -0.1875 to 0.1875
- leaf_basis: float32 [8192, 1024], P('leaf'), may hold values from -0.1875 to 0.1875
- leaf_back: float32 [32768, 256], P('leaf'), may hold values from -0.375 to 0.375
- level_one: float32 [8192, 1024], P('leaf'), may hold values from -0.25 to 0.25
- level_two: float32 [4096, 1024], P('leaf'), may hold values from -0.25 to 0.25
- level_three: float32 [2048, 1024], P('leaf'), may hold values from -0.25 to 0.25
- top_inverse: float32 [1024, 1024], P('leaf'), may hold values from -0.1 to 0.1, as said below
Outputs:
- solution: float32 [32768, 2048], P('leaf')
The draws below stay inside these ranges and needn't reach their ends.
Inputs may be any that keep to these rules, and one draw needn't show every extreme that they name: top_inverse is symmetric.
All inputs are finite; a program needn't handle non-finite values.
Results may differ from the reference program's by a relative error of at most 0.0001.
Values sent between devices are 32-bit elements; how exact they have to be, the bound alone decides.
A program may use at most 128 MiB of HBM per device.

```python
import math
import jax
import jax.numpy as jnp
from jax import lax

LEAF_ROWS = 1024
LOW_RANK = 256
SHOT_COUNT = 2048
TOP_NODES = 4
N_LEAF = 32


def draw_top_inverse(key, part):
    order = TOP_NODES * LOW_RANK
    entries = jax.random.normal(key, (order, order), jnp.float32)
    symmetric = (entries + entries.T) * (0.5 ** 0.5 / math.sqrt(order))
    return jnp.clip(symmetric, -0.1, 0.1)


def block_scale(key, shape, cuts, smallest, largest):
    level, own = 1.0, jax.random.fold_in(key, 6)
    for axis_at, parts in cuts:
        draws = jnp.exp(jax.random.uniform(jax.random.fold_in(own, axis_at), (parts,), jnp.float32, smallest / len(cuts), largest / len(cuts)))
        level = level * jnp.repeat(draws, shape[axis_at] // parts).reshape([-1 if axis == axis_at else 1 for axis in range(len(shape))])
    return level


def gaussian(rng, extent, scale, bound, split=(), held_as=jnp.bfloat16):
    values = jax.random.normal(rng, extent, jnp.float32) * scale
    if len(split) > 0:
        values = block_scale(rng, extent, split, -0.22, 0.18) * values
    return jnp.clip(values, min=-bound, max=bound).astype(held_as)


def setup_inputs(seed: int = 0) -> dict:
    streams_of = jax.random.split(jax.random.key(seed), 9)
    shots = gaussian(streams_of[0], (N_LEAF * LEAF_ROWS, SHOT_COUNT), 1.0, 6.0, ((0, 32),), jnp.float32)
    leaf_inverse = gaussian(streams_of[1], (N_LEAF * LEAF_ROWS, LEAF_ROWS), LEAF_ROWS ** -0.5, 0.1875, ((0, 32),), jnp.float32)
    leaf_basis = gaussian(streams_of[2], (N_LEAF * LOW_RANK, LEAF_ROWS), LEAF_ROWS ** -0.5, 0.1875, ((0, 32),), jnp.float32)
    leaf_back = gaussian(streams_of[3], (N_LEAF * LEAF_ROWS, LOW_RANK), LOW_RANK ** -0.5, 0.375, ((0, 32),), jnp.float32)
    level_one = gaussian(streams_of[4], (N_LEAF * LOW_RANK, 4 * LOW_RANK), (2 * LOW_RANK) ** -0.5, 0.25, ((0, 32),), jnp.float32)
    level_two = gaussian(streams_of[5], (N_LEAF * LOW_RANK // 2, 4 * LOW_RANK), (2 * LOW_RANK) ** -0.5, 0.25, ((0, 32),), jnp.float32)
    level_three = gaussian(streams_of[6], (N_LEAF * LOW_RANK // 4, 4 * LOW_RANK), (2 * LOW_RANK) ** -0.5, 0.25, ((0, 32),), jnp.float32)
    top_inverse = draw_top_inverse(jax.random.fold_in(streams_of[8], 71), 0)
    return {"shots": shots, "leaf_inverse": leaf_inverse, "leaf_basis": leaf_basis, "leaf_back": leaf_back, "level_one": level_one, "level_two": level_two, "level_three": level_three, "top_inverse": top_inverse}


def reference(shots, leaf_inverse, leaf_basis, leaf_back, level_one, level_two, level_three, top_inverse):
    highest = lax.Precision.HIGHEST
    leaves = N_LEAF
    rhs_blocks = shots.reshape(leaves, LEAF_ROWS, SHOT_COUNT)
    eliminators = leaf_inverse.reshape(leaves, LEAF_ROWS, LEAF_ROWS)
    solved = jnp.einsum("nij,njs->nis", eliminators, rhs_blocks, precision=highest)
    bases = leaf_basis.reshape(leaves, LOW_RANK, LEAF_ROWS)
    reduced = jnp.einsum("nrm,nms->nrs", bases, solved, precision=highest)
    stored = []
    for factors in (level_one, level_two, level_three):
        nodes = reduced.shape[0] // 2
        blocks = factors.reshape(nodes, 2 * LOW_RANK, 4 * LOW_RANK)
        inverse_block = blocks[:, :, :2 * LOW_RANK]
        reduce_block = blocks[:, :, 2 * LOW_RANK:3 * LOW_RANK]
        back_block = blocks[:, :, 3 * LOW_RANK:]
        stacked = reduced.reshape(nodes, 2 * LOW_RANK, SHOT_COUNT)
        coupled = jnp.einsum("nij,njs->nis", inverse_block, stacked, precision=highest)
        reduced = jnp.einsum("nir,nis->nrs", reduce_block, coupled, precision=highest)
        stored.append((coupled, back_block))
    gathered = reduced.reshape(TOP_NODES * LOW_RANK, SHOT_COUNT)
    top_solution = jnp.dot(top_inverse, gathered, precision=highest)
    coefficient = top_solution.reshape(TOP_NODES, LOW_RANK, SHOT_COUNT)
    for coupled, back_block in reversed(stored):
        remainder = coupled - jnp.einsum("nir,nrs->nis", back_block, coefficient, precision=highest)
        coefficient = remainder.reshape(-1, LOW_RANK, SHOT_COUNT)
    backs = leaf_back.reshape(leaves, LEAF_ROWS, LOW_RANK)
    result = solved - jnp.einsum("nmr,nrs->nms", backs, coefficient, precision=highest)
    return result.reshape(leaves * LEAF_ROWS, SHOT_COUNT)
```

```python
import functools

import jax
import jax.numpy as jnp
from jax import lax
from jax.experimental import pallas as pl
from jax.experimental.pallas import tpu as pltpu
from jax.sharding import PartitionSpec as P

LEVELS = 3
CHUNKS = 2
HIGH = lax.Precision.HIGH
MESH = pl.DeviceIdType.MESH
VMEM_LIMIT = 48 * 2**20


def dot(a, b):
    return jnp.dot(a, b, precision=HIGH, preferred_element_type=jnp.float32)


def dot_t(a, b):
    dims = (((0,), (0,)), ((), ()))
    return lax.dot_general(a, b, dims, precision=HIGH, preferred_element_type=jnp.float32)


def solve_kernel(
    sizes,
    shots, leaf_inverse, leaf_basis, leaf_back, level_one, level_two, level_three, top_inverse,
    out, w0,
    b, e, p, h, f1, f2, f3, top, a0, g1, g2, g3,
    c0send, c0, c1send, c1, c2send, c2, c3, call,
    z1, z2, z3, w2send, w2, w1send, w1, w0send,
    local_sem, send_sem, recv_sem,
):
    n, rank, nodes = sizes
    lanes1 = b.shape[3]
    lanes2, lanes3 = lanes1 // 2, lanes1 // 4
    me = lax.axis_index("leaf")
    core, x, y, z = me % 2, me // 2 % 2, me // 4 % 2, me // 8
    to_core = me + 1 - 2 * core
    to_x = me + 2 - 4 * x
    to_y = me + 4 - 8 * y
    z_of = lambda k: flip(z, k)
    to_z = [z_of(k) * 8 + me % 8 for k in range(1, nodes)]

    def ds(index, size):
        return pl.ds(pl.multiple_of(index * size, size), size)

    count = [0]
    local = {}

    def load(name, src, dst):
        local[name] = pltpu.make_async_copy(src, dst, local_sem.at[len(local)])
        local[name].start()

    remote = {}

    def send(name, src, dst, to):
        i = len(remote)
        remote[name] = pltpu.make_async_remote_copy(
            src_ref=src, dst_ref=dst, send_sem=send_sem.at[i], recv_sem=recv_sem.at[i],
            device_id=(to,), device_id_type=MESH,
        )
        remote[name].start()

    def arrived(name):
        remote[name].wait_recv()

    def columns(c, side):
        half = core if side == 0 else 1 - core
        return ds(c * 2 + half, lanes1)

    load("p", leaf_basis, p)
    load("e", leaf_inverse, e)
    load("b01", shots.at[:, columns(0, 1)], b.at[0, 1])
    load("b00", shots.at[:, columns(0, 0)], b.at[0, 0])
    rows1, rows2, rows3, rows4 = (r.shape[0] for r in (level_one, level_two, level_three, top_inverse))
    slot2, slot3 = x * 2 + core, y * 4 + x * 2 + core
    load("f1", level_one, f1.at[ds(core, rows1)])
    load("b11", shots.at[:, columns(1, 1)], b.at[1, 1])
    load("b10", shots.at[:, columns(1, 0)], b.at[1, 0])
    load("f2", level_two, f2.at[ds(slot2, rows2)])
    load("f3", level_three, f3.at[ds(slot3, rows3)])
    load("top", top_inverse, top.at[ds(slot3, rows4)])
    load("h", leaf_back, h)

    barrier = pltpu.get_barrier_semaphore()
    peers = [to_core, to_x, to_y] + to_z
    for peer in peers:
        pl.semaphore_signal(barrier, inc=1, device_id=(peer,), device_id_type=MESH)
    pl.semaphore_wait(barrier, len(peers))

    kq, fc = pl.ds(0, 3 * rank), pl.ds(3 * rank, rank)
    slot2x = (1 - x) * 2 + core
    slot3x, slot3y = y * 4 + (1 - x) * 2 + core, (1 - y) * 4 + x * 2 + core
    slot3xy = (1 - y) * 4 + (1 - x) * 2 + core
    send("f1", level_one, f1.at[ds(core, rows1)], to_core)
    send("f2x", level_two.at[:, kq], f2.at[ds(slot2, rows2), kq], to_x)
    send("f3y", level_three.at[:, kq], f3.at[ds(slot3, rows3), kq], to_y)
    send("f3x", level_three.at[:, kq], f3.at[ds(slot3, rows3), kq], to_x)
    send("f2c", level_two, f2.at[ds(slot2, rows2)], to_core)
    send("f3c", level_three, f3.at[ds(slot3, rows3)], to_core)
    send("tc", top_inverse, top.at[ds(slot3, rows4)], to_core)
    send("ty", top_inverse, top.at[ds(slot3, rows4)], to_y)
    send("f3fy", level_three.at[:, fc], f3.at[ds(slot3, rows3), fc], to_y)

    def forward(name, buf, slot, rows, cols, to):
        view = buf.at[ds(slot, rows), cols]
        send(name, view, view, to)

    local["p"].wait()
    local["e"].wait()
    a0[...] = dot(p[...], e[...])
    for c in range(CHUNKS):
        local[f"b{c}1"].wait()
        c0send[c] = dot(a0[...], b[c, 1])
        send(f"c0_{c}", c0send.at[c], c0.at[c, ds(core, rank)], to_core)
        local[f"b{c}0"].wait()
        c0[c, ds(core, rank), :] = dot(a0[...], b[c, 0])

    local["f1"].wait()
    arrived("f1")
    g1[...] = dot_t(f1[:, 2 * rank : 3 * rank], f1[:, : 2 * rank])
    for c in range(CHUNKS):
        arrived(f"c0_{c}")
        c1send[c] = dot(g1[...], c0[c, :, ds(1 - x, lanes2)])
        for part, half in enumerate((1 - y, y)):
            cols = ds(half, lanes3)
            send(f"c1_{c}{part}", c1send.at[c, :, cols], c1.at[c, ds(x, rank), cols], to_x)
        c1[c, ds(x, rank), :] = dot(g1[...], c0[c, :, ds(x, lanes2)])
    send("tx", top_inverse, top.at[ds(slot3, rows4)], to_x)
    send("f3fx", level_three.at[:, fc], f3.at[ds(slot3, rows3), fc], to_x)
    send("f2fx", level_two.at[:, fc], f2.at[ds(slot2, rows2), fc], to_x)

    def leaf_piece(c, side, part):
        cols = pl.ds(part * lanes2, lanes2)
        out[c, side, :, cols] = dot(e[...], b[c, side, :, cols])

    def z1_piece(c):
        z1[c] = dot(f1[:, : 2 * rank], c0[c])

    z1_piece(0)
    arrived("f3y")
    forward("f3yc", f3, slot3y, rows3, kq, to_core)
    z1_piece(1)
    arrived("f2x")
    forward("f2xc", f2, slot2x, rows2, kq, to_core)
    leaf_piece(0, 0, 0)
    local["f2"].wait()
    arrived("f2c")
    arrived("f2xc")
    g2[...] = dot_t(f2[:, 2 * rank : 3 * rank], f2[:, : 2 * rank])
    leaf_piece(0, 0, 1)
    arrived("f3x")
    forward("f3xy", f3, slot3x, rows3, kq, to_y)
    forward("f3xc", f3, slot3x, rows3, kq, to_core)
    arrived("ty")
    forward("tyc", top, slot3y, rows4, pl.ds(0, top.shape[1]), to_core)
    arrived("f3fy")
    forward("f3fyc", f3, slot3y, rows3, fc, to_core)
    leaf_piece(0, 1, 0)

    def up_two(c, part):
        arrived(f"c1_{c}{part}")
        if part == 0:
            cols = ds(1 - y, lanes3)
            c2send[c] = dot(g2[...], c1[c, :, cols])
            send(f"c2_{c}", c2send.at[c], c2.at[c, ds(y, rank)], to_y)
        else:
            c2[c, ds(y, rank), :] = dot(g2[...], c1[c, :, ds(y, lanes3)])

    def up_three(c):
        arrived(f"c2_{c}")
        c3[c] = dot(g3[...], c2[c])
        call[c, ds(z, rank), :] = c3[c]
        for k in range(1, nodes):
            send(f"c3_{c}{k}", c3.at[c], call.at[c, ds(z, rank)], to_z[k - 1])

    up_two(0, 0)
    leaf_piece(0, 1, 1)
    up_two(0, 1)
    arrived("f3xy")
    forward("f3xyc", f3, slot3xy, rows3, kq, to_core)
    z2[0] = dot(f2[:, : 2 * rank], c1[0])
    local["f3"].wait()
    for name in ("f3c", "f3yc", "f3xc", "f3xyc"):
        arrived(name)
    g3[...] = dot_t(f3[:, 2 * rank : 3 * rank], f3[:, : 2 * rank])
    up_three(0)
    up_two(1, 0)
    z3[0] = dot(f3[:, : 2 * rank], c2[0])
    up_two(1, 1)
    leaf_piece(1, 0, 0)
    arrived("tx")
    cols4 = pl.ds(0, top.shape[1])
    forward("txy", top, slot3x, rows4, cols4, to_y)
    forward("txc", top, slot3x, rows4, cols4, to_core)
    up_three(1)
    arrived("f3fx")
    forward("f3fxy", f3, slot3x, rows3, fc, to_y)
    forward("f3fxc", f3, slot3x, rows3, fc, to_core)
    z2[1] = dot(f2[:, : 2 * rank], c1[1])
    z3[1] = dot(f3[:, : 2 * rank], c2[1])
    leaf_piece(1, 0, 1)
    arrived("f2fx")
    forward("f2fxc", f2, slot2x, rows2, fc, to_core)
    arrived("txy")
    forward("txyc", top, slot3xy, rows4, cols4, to_core)
    arrived("f3fxy")
    forward("f3fxyc", f3, slot3xy, rows3, fc, to_core)
    local["top"].wait()
    for name in ("tc", "tyc", "txc", "txyc"):
        arrived(name)

    def down_three(c):
        for k in range(1, nodes):
            arrived(f"c3_{c}{k}")
        w3 = dot(top[...], call[c])
        other = pl.ds(pl.multiple_of((1 - y) * rank, rank), rank)
        own = pl.ds(pl.multiple_of(y * rank, rank), rank)
        w2send[c] = z3[c, other, :] - dot(f3[other, 3 * rank :], w3)
        send(f"w2_{c}", w2send.at[c], w2.at[c, :, ds(y, lanes3)], to_y)
        w2[c, :, ds(y, lanes3)] = z3[c, own, :] - dot(f3[own, 3 * rank :], w3)

    def down_two(c, part):
        half = y if part == 0 else 1 - y
        if part == 1:
            arrived(f"w2_{c}")
        cols = ds(half, lanes3)
        lanes = pl.ds(pl.multiple_of(x * lanes2 + half * lanes3, lanes3), lanes3)
        other = pl.ds(pl.multiple_of((1 - x) * rank, rank), rank)
        own = pl.ds(pl.multiple_of(x * rank, rank), rank)
        w1send[c, :, cols] = z2[c, other, cols] - dot(f2[other, 3 * rank :], w2[c, :, cols])
        send(f"w1_{c}{part}", w1send.at[c, :, cols], w1.at[c, :, lanes], to_x)
        w1[c, :, lanes] = z2[c, own, cols] - dot(f2[own, 3 * rank :], w2[c, :, cols])

    def down_one(c, part):
        half = x if part == 0 else 1 - x
        if part == 1:
            arrived(f"w1_{c}0")
            arrived(f"w1_{c}1")
        lanes = ds(half, lanes2)
        other = pl.ds(pl.multiple_of((1 - core) * rank, rank), rank)
        own = pl.ds(pl.multiple_of(core * rank, rank), rank)
        w0send[c, :, lanes] = z1[c, other, lanes] - dot(f1[other, 3 * rank :], w1[c, :, lanes])
        send(f"w0_{c}{part}", w0send.at[c, :, lanes], w0.at[c, 1, :, lanes], to_core)
        w0[c, 0, :, lanes] = z1[c, own, lanes] - dot(f1[own, 3 * rank :], w1[c, :, lanes])

    leaf_piece(1, 1, 0)
    for name in ("f3fyc", "f3fxc", "f3fxyc", "f2fxc"):
        arrived(name)
    down_three(0)
    down_two(0, 0)
    leaf_piece(1, 1, 1)
    down_two(0, 1)
    down_one(0, 0)
    down_three(1)
    down_two(1, 0)
    down_one(0, 1)
    down_two(1, 1)
    down_one(1, 0)
    local["h"].wait()
    out[0, 0] = out[0, 0] - dot(h[...], w0[0, 0])
    arrived("w0_00")
    arrived("w0_01")
    out[0, 1] = out[0, 1] - dot(h[...], w0[0, 1])
    down_one(1, 1)
    arrived("w0_10")
    arrived("w0_11")
    for copy in remote.values():
        copy.wait_send()


def flip(value, mask):
    bit = 1
    while bit <= mask:
        if mask & bit:
            value = value + bit - 2 * bit * (value // bit % 2)
        bit *= 2
    return value


def finish_kernel(part, w0, h, out, done, sem):
    me = lax.axis_index("leaf")
    core = me % 2
    lanes1 = part.shape[3]

    def store(src, c, side):
        half = core if side == 0 else 1 - core
        cols = pl.ds(pl.multiple_of((c * 2 + half) * lanes1, lanes1), lanes1)
        copy = pltpu.make_async_copy(src, out.at[:, cols], sem.at[c * 2 + side])
        copy.start()
        return copy

    copies = [store(part.at[0, side], 0, side) for side in range(2)]
    for side in range(2):
        done[side] = part[1, side] - dot(h[...], w0[1, side])
        copies.append(store(done.at[side], 1, side))
    for copy in copies:
        copy.wait()


def shards(n, *args):
    shots, leaf_inverse, leaf_basis, leaf_back, level_one, level_two, level_three, top_inverse = args
    rank, rows = leaf_basis.shape
    nodes = n // 2**LEVELS
    width = shots.shape[1] // CHUNKS
    l1, l2, l3 = width // 2, width // 4, width // 8
    f32 = jnp.float32
    vmem = lambda *shape: pltpu.VMEM(shape, f32)
    remote_count = 64 + 2 * nodes
    part, w0 = pl.pallas_call(
        functools.partial(solve_kernel, (n, rank, nodes)),
        name="solve",
        out_shape=(
            pltpu.VMEM((CHUNKS, 2, rows, l1), f32),
            pltpu.VMEM((CHUNKS, 2, rank, l1), f32),
        ),
        in_specs=[pl.BlockSpec(memory_space=pl.ANY)] * 8,
        out_specs=[pl.BlockSpec(memory_space=pltpu.VMEM)] * 2,
        scratch_shapes=[
            vmem(CHUNKS, 2, rows, l1),
            vmem(*leaf_inverse.shape),
            vmem(*leaf_basis.shape),
            vmem(*leaf_back.shape),
            vmem(2 * rank, 4 * rank),
            vmem(2 * rank, 4 * rank),
            vmem(2 * rank, 4 * rank),
            vmem(rank, nodes * rank),
            vmem(rank, rows),
            vmem(rank, 2 * rank),
            vmem(rank, 2 * rank),
            vmem(rank, 2 * rank),
            vmem(CHUNKS, rank, l1),
            vmem(CHUNKS, 2 * rank, l1),
            vmem(CHUNKS, rank, l2),
            vmem(CHUNKS, 2 * rank, l2),
            vmem(CHUNKS, rank, l3),
            vmem(CHUNKS, 2 * rank, l3),
            vmem(CHUNKS, rank, l3),
            vmem(CHUNKS, nodes * rank, l3),
            vmem(CHUNKS, 2 * rank, l1),
            vmem(CHUNKS, 2 * rank, l2),
            vmem(CHUNKS, 2 * rank, l3),
            vmem(CHUNKS, rank, l3),
            vmem(CHUNKS, rank, l2),
            vmem(CHUNKS, rank, l2),
            vmem(CHUNKS, rank, l1),
            vmem(CHUNKS, rank, l1),
            pltpu.SemaphoreType.DMA((16,)),
            pltpu.SemaphoreType.DMA((remote_count,)),
            pltpu.SemaphoreType.DMA((remote_count,)),
        ],
        compiler_params=pltpu.CompilerParams(
            collective_id=0, has_side_effects=True, vmem_limit_bytes=VMEM_LIMIT
        ),
    )(*args)
    return pl.pallas_call(
        finish_kernel,
        name="finish",
        out_shape=jax.ShapeDtypeStruct(shots.shape, f32),
        in_specs=[pl.BlockSpec(memory_space=pltpu.VMEM)] * 3,
        out_specs=pl.BlockSpec(memory_space=pl.ANY),
        scratch_shapes=[vmem(2, rows, l1), pltpu.SemaphoreType.DMA((4,))],
        compiler_params=pltpu.CompilerParams(vmem_limit_bytes=24 * 2**20),
    )(part, w0, leaf_back)


def solution(mesh):
    return jax.shard_map(
        functools.partial(shards, mesh.shape["leaf"]),
        mesh=mesh,
        in_specs=(P("leaf", None),) * 8,
        out_specs=P("leaf", None),
        check_vma=False,
    )
```

```python
import functools

import jax
import jax.numpy as jnp
from jax import lax
from jax.experimental import pallas as pl
from jax.experimental.pallas import tpu as pltpu
from jax.sharding import PartitionSpec as P

LEVELS = 3
CHUNKS = 2
DEPTHS = 2
HIGH = lax.Precision.HIGH
MESH = pl.DeviceIdType.MESH
VMEM_LIMIT = 48 * 2**20


def dot(a, b):
    return jnp.dot(a, b, precision=HIGH, preferred_element_type=jnp.float32)


def dot_t(a, b):
    dims = (((0,), (0,)), ((), ()))
    return lax.dot_general(a, b, dims, precision=HIGH, preferred_element_type=jnp.float32)


def halves(rows):
    return [pl.ds(i * (rows // 2), rows // 2) for i in range(2)]


def product(dst, a, b, minus=None):
    for rows in halves(dst.shape[0]):
        term = dot(a[rows], b)
        dst[rows, :] = term if minus is None else minus[rows, :] - term


def solve_kernel(
    sizes,
    shots, leaf_inverse, leaf_basis, leaf_back, level_one, level_two, level_three, top_inverse,
    out, w0,
    b, e, p, h, f1, f2, f3, top, a0, g1, g2, g3,
    c0send, c0, c1send, c1, c2send, c2, call,
    z1, z2, z3, w3, w2send, w2, w1send, w1, w0send,
    local_sem, send_sem, recv_sem, z_send, z_recv,
):
    n, rank, nodes = sizes
    lanes1 = b.shape[3]
    lanes2, lanes3 = lanes1 // 2, lanes1 // 4
    me = lax.axis_index("leaf")
    core, x, y, z = me % 2, me // 2 % 2, me // 4 % 2, me // 8
    to_core = me + 1 - 2 * core
    to_x = me + 2 - 4 * x
    to_y = me + 4 - 8 * y
    to_z = {k: me + 8 * (flip_of(z, k) - z) for k in range(1, nodes)}
    inner = (z % 4 == 1) | (z % 4 == 2)
    def ds(index, size):
        return pl.ds(pl.multiple_of(index * size, size), size)

    count = [0]
    local = {}

    def load(name, src, dst):
        local[name] = pltpu.make_async_copy(src, dst, local_sem.at[len(local)])
        local[name].start()

    remote = {}

    def send(name, src, dst, to):
        prepare(name, src, dst, to)
        remote[name].start()

    def prepare(name, src, dst, to):
        i = len(remote)
        remote[name] = pltpu.make_async_remote_copy(
            src_ref=src, dst_ref=dst, send_sem=send_sem.at[i], recv_sem=recv_sem.at[i],
            device_id=(to,), device_id_type=MESH,
        )

    def arrived(name):
        remote[name].wait_recv()

    def columns(c, side):
        half = core if side == 0 else 1 - core
        return ds(c * 2 + half, lanes1)

    load("p", leaf_basis, p)
    load("e", leaf_inverse, e)
    load("b01", shots.at[:, columns(0, 1)], b.at[0, 1])
    load("b00", shots.at[:, columns(0, 0)], b.at[0, 0])
    rows1, rows2, rows3, rows4 = (r.shape[0] for r in (level_one, level_two, level_three, top_inverse))
    slot2, slot3 = x * 2 + core, y * 4 + x * 2 + core
    load("f1", level_one, f1.at[ds(core, rows1)])
    load("b11", shots.at[:, columns(1, 1)], b.at[1, 1])
    load("b10", shots.at[:, columns(1, 0)], b.at[1, 0])
    load("f2", level_two, f2.at[ds(slot2, rows2)])
    load("f3", level_three, f3.at[ds(slot3, rows3)])
    load("top", top_inverse, top.at[ds(slot3, rows4)])
    load("h", leaf_back, h)

    barrier = pltpu.get_barrier_semaphore()

    def between(k):
        return inner if k == 3 else None

    def guarded(condition, action):
        action() if condition is None else pl.when(condition)(action)

    def greet(peer):
        pl.semaphore_signal(barrier, inc=1, device_id=(peer,), device_id_type=MESH)

    for peer in (to_core, to_x, to_y):
        greet(peer)
    for k, peer in to_z.items():
        guarded(between(k), functools.partial(greet, peer))
    far = 1 - inner.astype(jnp.int32) if nodes > 3 else 0
    pl.semaphore_wait(barrier, 3 + len(to_z) - far)

    kq, fc = pl.ds(0, 3 * rank), pl.ds(3 * rank, rank)
    slot2x = (1 - x) * 2 + core
    slot3x, slot3y = y * 4 + (1 - x) * 2 + core, (1 - y) * 4 + x * 2 + core
    slot3xy = (1 - y) * 4 + (1 - x) * 2 + core
    send("f1", level_one, f1.at[ds(core, rows1)], to_core)
    send("f3y", level_three.at[:, kq], f3.at[ds(slot3, rows3), kq], to_y)
    send("f3x", level_three.at[:, kq], f3.at[ds(slot3, rows3), kq], to_x)
    send("f2x", level_two.at[:, kq], f2.at[ds(slot2, rows2), kq], to_x)
    send("f2c", level_two, f2.at[ds(slot2, rows2)], to_core)
    send("f3c", level_three, f3.at[ds(slot3, rows3)], to_core)
    send("tc", top_inverse, top.at[ds(slot3, rows4)], to_core)

    def forward(name, buf, slot, rows, cols, to):
        view = buf.at[ds(slot, rows), cols]
        send(name, view, view, to)

    cols4 = pl.ds(0, top.shape[1])
    share = ((top, rows4, cols4), (f3, rows3, fc))
    for name, (buf, rows, cols) in zip(("t", "f"), share):
        src = top_inverse if name == "t" else level_three.at[:, fc]
        prepare(name + "x", src, buf.at[ds(slot3, rows), cols], to_x)
        view = buf.at[ds(slot3x, rows), cols]
        prepare(name + "xy", view, view, to_y)
        prepare(name + "xc", view, view, to_core)

    def forward_late():
        for name in "tf":
            remote[name + "x"].wait_recv()
            remote[name + "xy"].start()
            remote[name + "xc"].start()

    local["p"].wait()
    local["e"].wait()
    a0[...] = dot(p[...], e[...])
    for c in range(CHUNKS):
        local[f"b{c}1"].wait()
        c0send[c] = dot(a0[...], b[c, 1])
        send(f"c0_{c}", c0send.at[c], c0.at[c, ds(core, rank)], to_core)
        local[f"b{c}0"].wait()
        c0[c, ds(core, rank), :] = dot(a0[...], b[c, 0])

    def pieces(first, last):
        def piece(i, carry):
            i, part = i // DEPTHS, i % DEPTHS
            rows = pl.ds(pl.multiple_of(i % 2 * half_leaf, half_leaf), half_leaf)
            depth = ds(part, e.shape[1] // DEPTHS)
            c, side = i // 4, i // 2 % 2
            total = jnp.where(part == 0, 0.0, out[c, side, rows, :])
            out[c, side, rows, :] = total + dot(e[rows, depth], b[c, side, depth, :])
            return carry

        lax.fori_loop(DEPTHS * first, DEPTHS * last, piece, 0)

    half_leaf = e.shape[0] // 2

    def z1_piece(c):
        z1[c] = dot(f1[:, : 2 * rank], c0[c])

    local["f1"].wait()
    arrived("f1")
    g1[...] = dot_t(f1[:, 2 * rank : 3 * rank], f1[:, : 2 * rank])
    pieces(0, core)
    arrived("f3x")
    forward("f3xy", f3, slot3x, rows3, kq, to_y)
    forward("f3xc", f3, slot3x, rows3, kq, to_core)
    arrived("f3y")
    forward("f3yc", f3, slot3y, rows3, kq, to_core)
    send("ty", top_inverse, top.at[ds(slot3, rows4)], to_y)
    send("f3fy", level_three.at[:, fc], f3.at[ds(slot3, rows3), fc], to_y)
    pieces(core, 4 * core)
    for c in range(CHUNKS):
        arrived(f"c0_{c}")
        product(c1send.at[c], g1, c0[c, :, ds(1 - x, lanes2)])
        for part, half in enumerate((1 - y, y)):
            cols = ds(half, lanes3)
            send(f"c1_{c}{part}", c1send.at[c, :, cols], c1.at[c, ds(x, rank), cols], to_x)
        if c == 0:
            remote["tx"].start()
            remote["fx"].start()
        product(c1.at[c, ds(x, rank)], g1, c0[c, :, ds(x, lanes2)])
    send("f2fx", level_two.at[:, fc], f2.at[ds(slot2, rows2), fc], to_x)

    pieces(4 * core, 3 + core)
    arrived("f3xy")
    forward("f3xyc", f3, slot3xy, rows3, kq, to_core)
    arrived("f2x")
    forward("f2xc", f2, slot2x, rows2, kq, to_core)
    z1_piece(0)
    local["f3"].wait()
    for name in ("f3c", "f3yc", "f3xc", "f3xyc"):
        arrived(name)
    g3[...] = dot_t(f3[:, 2 * rank : 3 * rank], f3[:, : 2 * rank])
    local["f2"].wait()
    arrived("f2c")
    arrived("f2xc")
    g2[...] = dot_t(f2[:, 2 * rank : 3 * rank], f2[:, : 2 * rank])

    def up_two(c, part):
        arrived(f"c1_{c}{part}")
        if part == 0:
            cols = ds(1 - y, lanes3)
            product(c2send.at[c], g2, c1[c, :, cols])
            send(f"c2_{c}", c2send.at[c], c2.at[c, ds(y, rank)], to_y)
        else:
            product(c2.at[c, ds(y, rank)], g2, c1[c, :, ds(y, lanes3)])

    def up_three(c):
        arrived(f"c2_{c}")
        product(call.at[c, ds(z, rank)], g3, c2[c])
        for k in sorted(to_z, key=lambda k: (k != 2, -k)):
            guarded(between(k), block(c, k).start)

    def block(c, k):
        view = call.at[c, ds(z, rank)]
        i = c * nodes + k
        return pltpu.make_async_remote_copy(
            src_ref=view, dst_ref=view, send_sem=z_send.at[i], recv_sem=z_recv.at[i],
            device_id=(to_z[k],), device_id_type=MESH,
        )

    def passed(c):
        view = call.at[c, ds(flip_of(z, 2), rank)]
        return pltpu.make_async_remote_copy(
            src_ref=view, dst_ref=view, send_sem=z_send.at[c * nodes], recv_sem=z_recv.at[c * nodes + 3],
            device_id=(to_z[1],), device_id_type=MESH,
        )

    def pass_on(c):
        if nodes > 3:
            @pl.when(inner)
            def _():
                block(c, 2).wait_recv()
                passed(c).start()

    def gathered(c):
        for k in to_z:
            guarded(~inner if k == 2 and nodes > 3 else None, block(c, k).wait_recv)

    up_two(0, 0)
    pieces(4 * core, 5 * core)
    up_two(0, 1)
    product(z2.at[0], f2.at[:, : 2 * rank], c1[0])
    arrived("ty")
    forward("tyc", top, slot3y, rows4, cols4, to_core)
    arrived("f3fy")
    forward("f3fyc", f3, slot3y, rows3, fc, to_core)
    pieces(3 + 2 * core, 4 + core)
    up_three(0)
    forward_late()
    product(z3.at[0], f3.at[:, : 2 * rank], c2[0])
    pieces(4 + core, 5 + core)
    up_two(1, 0)
    z1_piece(1)
    arrived("txy")
    forward("txyc", top, slot3xy, rows4, cols4, to_core)
    arrived("fxy")
    forward("fxyc", f3, slot3xy, rows3, fc, to_core)
    up_two(1, 1)
    pass_on(0)
    up_three(1)
    product(z3.at[1], f3.at[:, : 2 * rank], c2[1])
    pieces(5 + core, 6)
    product(z2.at[1], f2.at[:, : 2 * rank], c1[1])
    local["top"].wait()
    for name in ("tc", "tyc", "txc", "txyc", "f3fyc", "fxc", "fxyc"):
        arrived(name)

    def down_three(c):
        gathered(c)
        product(w3, top, call[c])
        other = pl.ds(pl.multiple_of((1 - y) * rank, rank), rank)
        own = pl.ds(pl.multiple_of(y * rank, rank), rank)
        product(w2send.at[c], f3.at[other, 3 * rank :], w3[...], z3.at[c, other])
        send(f"w2_{c}", w2send.at[c], w2.at[c, :, ds(y, lanes3)], to_y)
        product(w2.at[c, :, ds(y, lanes3)], f3.at[own, 3 * rank :], w3[...], z3.at[c, own])

    def down_two(c, part):
        half = y if part == 0 else 1 - y
        if part == 1:
            arrived(f"w2_{c}")
        cols = ds(half, lanes3)
        lanes = pl.ds(pl.multiple_of(x * lanes2 + half * lanes3, lanes3), lanes3)
        other = pl.ds(pl.multiple_of((1 - x) * rank, rank), rank)
        own = pl.ds(pl.multiple_of(x * rank, rank), rank)
        product(w1send.at[c, :, cols], f2.at[other, 3 * rank :], w2[c, :, cols], z2.at[c, other, cols])
        send(f"w1_{c}{part}", w1send.at[c, :, cols], w1.at[c, :, lanes], to_x)
        product(w1.at[c, :, lanes], f2.at[own, 3 * rank :], w2[c, :, cols], z2.at[c, own, cols])

    def down_one(c, part):
        half = x if part == 0 else 1 - x
        if part == 1:
            arrived(f"w1_{c}0")
            arrived(f"w1_{c}1")
        lanes = ds(half, lanes2)
        other = pl.ds(pl.multiple_of((1 - core) * rank, rank), rank)
        own = pl.ds(pl.multiple_of(core * rank, rank), rank)
        product(w0send.at[c, :, lanes], f1.at[other, 3 * rank :], w1[c, :, lanes], z1.at[c, other, lanes])
        send(f"w0_{c}{part}", w0send.at[c, :, lanes], w0.at[c, 1, :, lanes], to_core)
        product(w0.at[c, 0, :, lanes], f1.at[own, 3 * rank :], w1[c, :, lanes], z1.at[c, own, lanes])

    def last(c, side, half):
        lanes = ds(half, lanes2)
        product(out.at[c, side, :, lanes], h, w0[c, side, :, lanes], out.at[c, side, :, lanes])

    down_three(0)
    arrived("f2fx")
    forward("f2fxc", f2, slot2x, rows2, fc, to_core)
    pieces(6, 7)
    arrived("f2fxc")
    down_two(0, 0)
    pass_on(1)
    down_two(0, 1)
    down_one(0, 0)
    pieces(7, 8)
    down_three(1)
    down_two(1, 0)
    down_one(0, 1)
    local["h"].wait()
    last(0, 0, x)
    down_two(1, 1)
    down_one(1, 0)
    last(0, 0, 1 - x)
    arrived("w0_00")
    last(0, 1, x)
    last(1, 0, x)
    arrived("w0_10")
    last(1, 1, x)
    arrived("w0_01")
    last(0, 1, 1 - x)
    down_one(1, 1)
    last(1, 0, 1 - x)
    arrived("w0_11")
    for copy in remote.values():
        copy.wait_send()
    for c in range(CHUNKS):
        for k in to_z:
            guarded(between(k), block(c, k).wait_send)
        if nodes > 3:
            pl.when(inner)(passed(c).wait_send)


def flip_of(value, mask):
    bit = 1
    while bit <= mask:
        if mask & bit:
            value = value + bit - 2 * bit * (value // bit % 2)
        bit *= 2
    return value


def finish_kernel(part, w0, h, out, done, sem):
    me = lax.axis_index("leaf")
    core, x = me % 2, me // 2 % 2
    lanes1 = part.shape[3]
    lanes2 = lanes1 // 2
    copies = []

    def columns(c, side, half):
        start = c * 4 + (core if side == 0 else 1 - core) * 2 + half
        return pl.ds(pl.multiple_of(start * lanes2, lanes2), lanes2)

    def store(src, cols):
        copies.append(pltpu.make_async_copy(src, out.at[:, cols], sem.at[len(copies)]))
        copies[-1].start()

    for c in range(CHUNKS):
        for side in range(2):
            for half in (x, 1 - x):
                lanes = pl.ds(pl.multiple_of(half * lanes2, lanes2), lanes2)
                if len(copies) < 4 * CHUNKS - 1:
                    store(part.at[c, side, :, lanes], columns(c, side, half))
    for rows in halves(done.shape[0]):
        done[rows, :] = part[1, 1, rows, lanes] - dot(h[rows, :], w0[1, 1, :, lanes])
    store(done, columns(c, side, half))
    for copy in copies:
        copy.wait()


def shards(n, *args):
    shots, leaf_inverse, leaf_basis, leaf_back, level_one, level_two, level_three, top_inverse = args
    rank, rows = leaf_basis.shape
    nodes = n // 2**LEVELS
    width = shots.shape[1] // CHUNKS
    l1, l2, l3 = width // 2, width // 4, width // 8
    f32 = jnp.float32
    vmem = lambda *shape: pltpu.VMEM(shape, f32)
    z_count = CHUNKS * nodes
    part, w0 = pl.pallas_call(
        functools.partial(solve_kernel, (n, rank, nodes)),
        name="solve",
        out_shape=(
            pltpu.VMEM((CHUNKS, 2, rows, l1), f32),
            pltpu.VMEM((CHUNKS, 2, rank, l1), f32),
        ),
        in_specs=[pl.BlockSpec(memory_space=pl.ANY)] * 8,
        out_specs=[pl.BlockSpec(memory_space=pltpu.VMEM)] * 2,
        scratch_shapes=[
            vmem(CHUNKS, 2, rows, l1),
            vmem(*leaf_inverse.shape),
            vmem(*leaf_basis.shape),
            vmem(*leaf_back.shape),
            vmem(2 * rank, 4 * rank),
            vmem(2 * rank, 4 * rank),
            vmem(2 * rank, 4 * rank),
            vmem(rank, nodes * rank),
            vmem(rank, rows),
            vmem(rank, 2 * rank),
            vmem(rank, 2 * rank),
            vmem(rank, 2 * rank),
            vmem(CHUNKS, rank, l1),
            vmem(CHUNKS, 2 * rank, l1),
            vmem(CHUNKS, rank, l2),
            vmem(CHUNKS, 2 * rank, l2),
            vmem(CHUNKS, rank, l3),
            vmem(CHUNKS, 2 * rank, l3),
            vmem(CHUNKS, nodes * rank, l3),
            vmem(CHUNKS, 2 * rank, l1),
            vmem(CHUNKS, 2 * rank, l2),
            vmem(CHUNKS, 2 * rank, l3),
            vmem(rank, l3),
            vmem(CHUNKS, rank, l3),
            vmem(CHUNKS, rank, l2),
            vmem(CHUNKS, rank, l2),
            vmem(CHUNKS, rank, l1),
            vmem(CHUNKS, rank, l1),
            pltpu.SemaphoreType.DMA((16,)),
            pltpu.SemaphoreType.DMA((64,)),
            pltpu.SemaphoreType.DMA((64,)),
            pltpu.SemaphoreType.DMA((z_count,)),
            pltpu.SemaphoreType.DMA((z_count,)),
        ],
        compiler_params=pltpu.CompilerParams(
            collective_id=0, has_side_effects=True, vmem_limit_bytes=VMEM_LIMIT
        ),
    )(*args)
    return pl.pallas_call(
        finish_kernel,
        name="finish",
        out_shape=jax.ShapeDtypeStruct(shots.shape, f32),
        in_specs=[pl.BlockSpec(memory_space=pltpu.VMEM)] * 3,
        out_specs=pl.BlockSpec(memory_space=pl.ANY),
        scratch_shapes=[vmem(rows, l2), pltpu.SemaphoreType.DMA((4 * CHUNKS,))],
        compiler_params=pltpu.CompilerParams(vmem_limit_bytes=24 * 2**20),
    )(part, w0, leaf_back)


def solution(mesh):
    return jax.shard_map(
        functools.partial(shards, mesh.shape["leaf"]),
        mesh=mesh,
        in_specs=(P("leaf", None),) * 8,
        out_specs=P("leaf", None),
        check_vma=False,
    )
```

```python
import functools

import jax
import jax.numpy as jnp
from jax import lax
from jax.experimental import pallas as pl
from jax.experimental.pallas import tpu as pltpu
from jax.sharding import PartitionSpec as P

LEVELS = 3
CHUNKS = 2
DEPTHS = 2
HIGH = lax.Precision.HIGH
MESH = pl.DeviceIdType.MESH
VMEM_LIMIT = 48 * 2**20


def dot(a, b):
    return jnp.dot(a, b, precision=HIGH, preferred_element_type=jnp.float32)


def dot_t(a, b):
    dims = (((0,), (0,)), ((), ()))
    return lax.dot_general(a, b, dims, precision=HIGH, preferred_element_type=jnp.float32)


def halves(rows):
    return [pl.ds(i * (rows // 2), rows // 2) for i in range(2)]


def product(dst, a, b, minus=None):
    for rows in halves(dst.shape[0]):
        term = dot(a[rows], b)
        dst[rows, :] = term if minus is None else minus[rows, :] - term


def solve_kernel(
    sizes,
    shots, leaf_inverse, leaf_basis, leaf_back, level_one, level_two, level_three, top_inverse,
    out, w0,
    b, e, p, h, f1, f2, f3, top, a0, g1, g2, g3,
    c0send, c0, c1send, c1, c2send, c2, call,
    z1, z2, z3, w3, w2send, w2, w1send, w1, w0send,
    local_sem, send_sem, recv_sem, z_send, z_recv,
):
    n, rank, nodes = sizes
    lanes1 = b.shape[3]
    lanes2, lanes3 = lanes1 // 2, lanes1 // 4
    me = lax.axis_index("leaf")
    core, x, y, z = me % 2, me // 2 % 2, me // 4 % 2, me // 8
    to_core = me + 1 - 2 * core
    to_x = me + 2 - 4 * x
    to_y = me + 4 - 8 * y
    to_z = {k: me + 8 * (flip_of(z, k) - z) for k in range(1, nodes)}
    inner = (z % 4 == 1) | (z % 4 == 2)
    def ds(index, size):
        return pl.ds(pl.multiple_of(index * size, size), size)

    count = [0]
    local = {}

    def load(name, src, dst):
        local[name] = pltpu.make_async_copy(src, dst, local_sem.at[len(local)])
        local[name].start()

    remote = {}

    def send(name, src, dst, to):
        prepare(name, src, dst, to)
        remote[name].start()

    def prepare(name, src, dst, to):
        i = len(remote)
        remote[name] = pltpu.make_async_remote_copy(
            src_ref=src, dst_ref=dst, send_sem=send_sem.at[i], recv_sem=recv_sem.at[i],
            device_id=(to,), device_id_type=MESH,
        )

    def arrived(name):
        remote[name].wait_recv()

    def columns(c, side):
        half = core if side == 0 else 1 - core
        return ds(c * 2 + half, lanes1)

    load("p", leaf_basis, p)
    load("e", leaf_inverse, e)
    load("b01", shots.at[:, columns(0, 1)], b.at[0, 1])
    load("b00", shots.at[:, columns(0, 0)], b.at[0, 0])
    rows1, rows2, rows3, rows4 = (r.shape[0] for r in (level_one, level_two, level_three, top_inverse))
    slot2, slot3 = x * 2 + core, y * 4 + x * 2 + core
    load("f1", level_one, f1.at[ds(core, rows1)])
    load("b11", shots.at[:, columns(1, 1)], b.at[1, 1])
    load("b10", shots.at[:, columns(1, 0)], b.at[1, 0])
    load("f2", level_two, f2.at[ds(slot2, rows2)])
    load("f3", level_three, f3.at[ds(slot3, rows3)])
    load("top", top_inverse, top.at[ds(slot3, rows4)])
    load("h", leaf_back, h)

    barrier = pltpu.get_barrier_semaphore()

    def between(k):
        return inner if k == 3 else None

    def guarded(condition, action):
        action() if condition is None else pl.when(condition)(action)

    def greet(peer):
        pl.semaphore_signal(barrier, inc=1, device_id=(peer,), device_id_type=MESH)

    for peer in (to_core, to_x, to_y):
        greet(peer)
    for k, peer in to_z.items():
        guarded(between(k), functools.partial(greet, peer))
    far = 1 - inner.astype(jnp.int32) if nodes > 3 else 0
    pl.semaphore_wait(barrier, 3 + len(to_z) - far)

    kq, fc = pl.ds(0, 3 * rank), pl.ds(3 * rank, rank)
    slot2x = (1 - x) * 2 + core
    slot3x, slot3y = y * 4 + (1 - x) * 2 + core, (1 - y) * 4 + x * 2 + core
    slot3xy = (1 - y) * 4 + (1 - x) * 2 + core
    send("f1", level_one, f1.at[ds(core, rows1)], to_core)
    send("f3y", level_three.at[:, kq], f3.at[ds(slot3, rows3), kq], to_y)
    send("f3x", level_three.at[:, kq], f3.at[ds(slot3, rows3), kq], to_x)
    send("f2x", level_two.at[:, kq], f2.at[ds(slot2, rows2), kq], to_x)
    send("f2c", level_two, f2.at[ds(slot2, rows2)], to_core)
    send("f3c", level_three, f3.at[ds(slot3, rows3)], to_core)
    send("tc", top_inverse, top.at[ds(slot3, rows4)], to_core)

    def forward(name, buf, slot, rows, cols, to):
        view = buf.at[ds(slot, rows), cols]
        send(name, view, view, to)

    cols4 = pl.ds(0, top.shape[1])
    share = ((top, rows4, cols4), (f3, rows3, fc))
    for name, (buf, rows, cols) in zip(("t", "f"), share):
        src = top_inverse if name == "t" else level_three.at[:, fc]
        prepare(name + "x", src, buf.at[ds(slot3, rows), cols], to_x)
        view = buf.at[ds(slot3x, rows), cols]
        prepare(name + "xy", view, view, to_y)
        prepare(name + "xc", view, view, to_core)

    def forward_late():
        for name in "tf":
            remote[name + "x"].wait_recv()
            remote[name + "xy"].start()
            remote[name + "xc"].start()

    for name, buf, slot, rows in (("f3xy", f3, slot3xy, rows3), ("f2x", f2, slot2x, rows2)):
        view = buf.at[ds(slot, rows), kq]
        prepare(name + "c", view, view, to_core)

    def forward_kq(condition):
        @pl.when(condition)
        def _():
            for key in ("f3xy", "f2x"):
                remote[key].wait_recv()
                remote[key + "c"].start()

    local["p"].wait()
    local["e"].wait()
    a0[...] = dot(p[...], e[...])
    for c in range(CHUNKS):
        local[f"b{c}1"].wait()
        c0send[c] = dot(a0[...], b[c, 1])
        send(f"c0_{c}", c0send.at[c], c0.at[c, ds(core, rank)], to_core)
        local[f"b{c}0"].wait()
        c0[c, ds(core, rank), :] = dot(a0[...], b[c, 0])

    def pieces(first, last):
        def piece(i, carry):
            i, part = i // DEPTHS, i % DEPTHS
            rows = pl.ds(pl.multiple_of(i % 2 * half_leaf, half_leaf), half_leaf)
            depth = ds(part, e.shape[1] // DEPTHS)
            c, side = i // 4, i // 2 % 2
            total = jnp.where(part == 0, 0.0, out[c, side, rows, :])
            out[c, side, rows, :] = total + dot(e[rows, depth], b[c, side, depth, :])
            return carry

        lax.fori_loop(first, last, piece, 0)

    half_leaf = e.shape[0] // 2

    def z1_piece(c):
        z1[c] = dot(f1[:, : 2 * rank], c0[c])

    local["f1"].wait()
    arrived("f1")
    g1[...] = dot_t(f1[:, 2 * rank : 3 * rank], f1[:, : 2 * rank])
    pieces(0, 2 * core)
    arrived("f3x")
    forward("f3xy", f3, slot3x, rows3, kq, to_y)
    forward("f3xc", f3, slot3x, rows3, kq, to_core)
    arrived("f3y")
    forward("f3yc", f3, slot3y, rows3, kq, to_core)
    send("ty", top_inverse, top.at[ds(slot3, rows4)], to_y)
    send("f3fy", level_three.at[:, fc], f3.at[ds(slot3, rows3), fc], to_y)
    pieces(2 * core, 7 * core)
    forward_kq(core == 1)
    for c in range(CHUNKS):
        arrived(f"c0_{c}")
        product(c1send.at[c], g1, c0[c, :, ds(1 - x, lanes2)])
        for part, half in enumerate((1 - y, y)):
            cols = ds(half, lanes3)
            send(f"c1_{c}{part}", c1send.at[c, :, cols], c1.at[c, ds(x, rank), cols], to_x)
        product(c1.at[c, ds(x, rank)], g1, c0[c, :, ds(x, lanes2)])
    remote["tx"].start()
    remote["fx"].start()
    send("f2fx", level_two.at[:, fc], f2.at[ds(slot2, rows2), fc], to_x)

    def up_two(c, part):
        arrived(f"c1_{c}{part}")
        if part == 0:
            cols = ds(1 - y, lanes3)
            product(c2send.at[c], g2, c1[c, :, cols])
            send(f"c2_{c}", c2send.at[c], c2.at[c, ds(y, rank)], to_y)
        else:
            product(c2.at[c, ds(y, rank)], g2, c1[c, :, ds(y, lanes3)])

    def up_three(c):
        arrived(f"c2_{c}")
        product(call.at[c, ds(z, rank)], g3, c2[c])
        for k in sorted(to_z, key=lambda k: (k != 2, -k)):
            guarded(between(k), block(c, k).start)

    def block(c, k):
        view = call.at[c, ds(z, rank)]
        i = c * nodes + k
        return pltpu.make_async_remote_copy(
            src_ref=view, dst_ref=view, send_sem=z_send.at[i], recv_sem=z_recv.at[i],
            device_id=(to_z[k],), device_id_type=MESH,
        )

    def passed(c):
        view = call.at[c, ds(flip_of(z, 2), rank)]
        return pltpu.make_async_remote_copy(
            src_ref=view, dst_ref=view, send_sem=z_send.at[c * nodes], recv_sem=z_recv.at[c * nodes + 3],
            device_id=(to_z[1],), device_id_type=MESH,
        )

    def pass_on(c):
        if nodes > 3:
            @pl.when(inner)
            def _():
                block(c, 2).wait_recv()
                passed(c).start()

    def gathered(c):
        for k in to_z:
            guarded(~inner if k == 2 and nodes > 3 else None, block(c, k).wait_recv)

    pieces(7 * core, 6 + core)
    forward_kq(core == 0)
    local["f2"].wait()
    arrived("f2c")
    arrived("f2xc")
    g2[...] = dot_t(f2[:, 2 * rank : 3 * rank], f2[:, : 2 * rank])
    up_two(0, 0)
    local["f3"].wait()
    for name in ("f3c", "f3yc", "f3xc", "f3xyc"):
        arrived(name)
    g3[...] = dot_t(f3[:, 2 * rank : 3 * rank], f3[:, : 2 * rank])
    z1_piece(0)
    pieces(7 * core, 9 * core)
    up_two(0, 1)
    product(z2.at[0], f2.at[:, : 2 * rank], c1[0])
    arrived("ty")
    forward("tyc", top, slot3y, rows4, cols4, to_core)
    arrived("f3fy")
    forward("f3fyc", f3, slot3y, rows3, fc, to_core)
    pieces(6 + 3 * core, 8 + core)
    up_three(0)
    product(z3.at[0], f3.at[:, : 2 * rank], c2[0])
    up_two(1, 0)
    z1_piece(1)
    up_two(1, 1)
    pieces(8 + core, 10 + core)
    forward_late()
    pass_on(0)
    up_three(1)
    product(z3.at[1], f3.at[:, : 2 * rank], c2[1])
    product(z2.at[1], f2.at[:, : 2 * rank], c1[1])
    pieces(10 + core, 12 + core)
    arrived("txy")
    forward("txyc", top, slot3xy, rows4, cols4, to_core)
    arrived("fxy")
    forward("fxyc", f3, slot3xy, rows3, fc, to_core)
    arrived("f2fx")
    forward("f2fxc", f2, slot2x, rows2, fc, to_core)
    local["top"].wait()
    for name in ("tc", "tyc", "txc", "txyc", "f3fyc", "fxc", "fxyc"):
        arrived(name)

    def down_three(c):
        gathered(c)
        product(w3, top, call[c])
        other = pl.ds(pl.multiple_of((1 - y) * rank, rank), rank)
        own = pl.ds(pl.multiple_of(y * rank, rank), rank)
        product(w2send.at[c], f3.at[other, 3 * rank :], w3[...], z3.at[c, other])
        send(f"w2_{c}", w2send.at[c], w2.at[c, :, ds(y, lanes3)], to_y)
        product(w2.at[c, :, ds(y, lanes3)], f3.at[own, 3 * rank :], w3[...], z3.at[c, own])

    def down_two(c, part):
        half = y if part == 0 else 1 - y
        if part == 1:
            arrived(f"w2_{c}")
        cols = ds(half, lanes3)
        lanes = pl.ds(pl.multiple_of(x * lanes2 + half * lanes3, lanes3), lanes3)
        other = pl.ds(pl.multiple_of((1 - x) * rank, rank), rank)
        own = pl.ds(pl.multiple_of(x * rank, rank), rank)
        product(w1send.at[c, :, cols], f2.at[other, 3 * rank :], w2[c, :, cols], z2.at[c, other, cols])
        send(f"w1_{c}{part}", w1send.at[c, :, cols], w1.at[c, :, lanes], to_x)
        product(w1.at[c, :, lanes], f2.at[own, 3 * rank :], w2[c, :, cols], z2.at[c, own, cols])

    def down_one(c, part):
        half = x if part == 0 else 1 - x
        if part == 1:
            arrived(f"w1_{c}0")
            arrived(f"w1_{c}1")
        lanes = ds(half, lanes2)
        other = pl.ds(pl.multiple_of((1 - core) * rank, rank), rank)
        own = pl.ds(pl.multiple_of(core * rank, rank), rank)
        product(w0send.at[c, :, lanes], f1.at[other, 3 * rank :], w1[c, :, lanes], z1.at[c, other, lanes])
        send(f"w0_{c}{part}", w0send.at[c, :, lanes], w0.at[c, 1, :, lanes], to_core)
        product(w0.at[c, 0, :, lanes], f1.at[own, 3 * rank :], w1[c, :, lanes], z1.at[c, own, lanes])

    def last(c, side, half):
        lanes = ds(half, lanes2)
        product(out.at[c, side, :, lanes], h, w0[c, side, :, lanes], out.at[c, side, :, lanes])

    down_three(0)
    arrived("f2fxc")
    down_two(0, 0)
    pass_on(1)
    pieces(12 + core, 14 + core)
    down_two(0, 1)
    down_one(0, 0)
    down_three(1)
    down_two(1, 0)
    pieces(14 + core, 16)
    down_one(0, 1)
    local["h"].wait()
    last(0, 0, x)
    down_two(1, 1)
    down_one(1, 0)
    last(0, 0, 1 - x)
    arrived("w0_00")
    last(0, 1, x)
    last(1, 0, x)
    arrived("w0_10")
    last(1, 1, x)
    arrived("w0_01")
    last(0, 1, 1 - x)
    down_one(1, 1)
    last(1, 0, 1 - x)
    arrived("w0_11")
    for copy in remote.values():
        copy.wait_send()
    for c in range(CHUNKS):
        for k in to_z:
            guarded(between(k), block(c, k).wait_send)
        if nodes > 3:
            pl.when(inner)(passed(c).wait_send)


def flip_of(value, mask):
    bit = 1
    while bit <= mask:
        if mask & bit:
            value = value + bit - 2 * bit * (value // bit % 2)
        bit *= 2
    return value


def finish_kernel(part, w0, h, out, done, sem):
    me = lax.axis_index("leaf")
    core, x = me % 2, me // 2 % 2
    lanes1 = part.shape[3]
    lanes2 = lanes1 // 2
    copies = []

    def columns(c, side, half):
        start = c * 4 + (core if side == 0 else 1 - core) * 2 + half
        return pl.ds(pl.multiple_of(start * lanes2, lanes2), lanes2)

    def store(src, cols):
        copies.append(pltpu.make_async_copy(src, out.at[:, cols], sem.at[len(copies)]))
        copies[-1].start()

    for c in range(CHUNKS):
        for side in range(2):
            for half in (x, 1 - x):
                lanes = pl.ds(pl.multiple_of(half * lanes2, lanes2), lanes2)
                if len(copies) < 4 * CHUNKS - 1:
                    store(part.at[c, side, :, lanes], columns(c, side, half))
    for rows in halves(done.shape[0]):
        done[rows, :] = part[1, 1, rows, lanes] - dot(h[rows, :], w0[1, 1, :, lanes])
    store(done, columns(c, side, half))
    for copy in copies:
        copy.wait()


def shards(n, *args):
    shots, leaf_inverse, leaf_basis, leaf_back, level_one, level_two, level_three, top_inverse = args
    rank, rows = leaf_basis.shape
    nodes = n // 2**LEVELS
    width = shots.shape[1] // CHUNKS
    l1, l2, l3 = width // 2, width // 4, width // 8
    f32 = jnp.float32
    vmem = lambda *shape: pltpu.VMEM(shape, f32)
    z_count = CHUNKS * nodes
    part, w0 = pl.pallas_call(
        functools.partial(solve_kernel, (n, rank, nodes)),
        name="solve",
        out_shape=(
            pltpu.VMEM((CHUNKS, 2, rows, l1), f32),
            pltpu.VMEM((CHUNKS, 2, rank, l1), f32),
        ),
        in_specs=[pl.BlockSpec(memory_space=pl.ANY)] * 8,
        out_specs=[pl.BlockSpec(memory_space=pltpu.VMEM)] * 2,
        scratch_shapes=[
            vmem(CHUNKS, 2, rows, l1),
            vmem(*leaf_inverse.shape),
            vmem(*leaf_basis.shape),
            vmem(*leaf_back.shape),
            vmem(2 * rank, 4 * rank),
            vmem(2 * rank, 4 * rank),
            vmem(2 * rank, 4 * rank),
            vmem(rank, nodes * rank),
            vmem(rank, rows),
            vmem(rank, 2 * rank),
            vmem(rank, 2 * rank),
            vmem(rank, 2 * rank),
            vmem(CHUNKS, rank, l1),
            vmem(CHUNKS, 2 * rank, l1),
            vmem(CHUNKS, rank, l2),
            vmem(CHUNKS, 2 * rank, l2),
            vmem(CHUNKS, rank, l3),
            vmem(CHUNKS, 2 * rank, l3),
            vmem(CHUNKS, nodes * rank, l3),
            vmem(CHUNKS, 2 * rank, l1),
            vmem(CHUNKS, 2 * rank, l2),
            vmem(CHUNKS, 2 * rank, l3),
            vmem(rank, l3),
            vmem(CHUNKS, rank, l3),
            vmem(CHUNKS, rank, l2),
            vmem(CHUNKS, rank, l2),
            vmem(CHUNKS, rank, l1),
            vmem(CHUNKS, rank, l1),
            pltpu.SemaphoreType.DMA((16,)),
            pltpu.SemaphoreType.DMA((64,)),
            pltpu.SemaphoreType.DMA((64,)),
            pltpu.SemaphoreType.DMA((z_count,)),
            pltpu.SemaphoreType.DMA((z_count,)),
        ],
        compiler_params=pltpu.CompilerParams(
            collective_id=0, has_side_effects=True, vmem_limit_bytes=VMEM_LIMIT
        ),
    )(*args)
    return pl.pallas_call(
        finish_kernel,
        name="finish",
        out_shape=jax.ShapeDtypeStruct(shots.shape, f32),
        in_specs=[pl.BlockSpec(memory_space=pltpu.VMEM)] * 3,
        out_specs=pl.BlockSpec(memory_space=pl.ANY),
        scratch_shapes=[vmem(rows, l2), pltpu.SemaphoreType.DMA((4 * CHUNKS,))],
        compiler_params=pltpu.CompilerParams(vmem_limit_bytes=24 * 2**20),
    )(part, w0, leaf_back)


def solution(mesh):
    return jax.shard_map(
        functools.partial(shards, mesh.shape["leaf"]),
        mesh=mesh,
        in_specs=(P("leaf", None),) * 8,
        out_specs=P("leaf", None),
        check_vma=False,
    )
```

```python
import functools

import jax
import jax.numpy as jnp
from jax import lax
from jax.experimental import pallas as pl
from jax.experimental.pallas import tpu as pltpu
from jax.sharding import PartitionSpec as P

LEVELS = 3
CHUNKS = 2
DEPTHS = 2
HIGH = lax.Precision.HIGH
MESH = pl.DeviceIdType.MESH
VMEM_LIMIT = 48 * 2**20


def dot(a, b):
    return jnp.dot(a, b, precision=HIGH, preferred_element_type=jnp.float32)


def dot_t(a, b):
    dims = (((0,), (0,)), ((), ()))
    return lax.dot_general(a, b, dims, precision=HIGH, preferred_element_type=jnp.float32)


def halves(rows):
    return [pl.ds(i * (rows // 2), rows // 2) for i in range(2)]


def product(dst, a, b, minus=None):
    for rows in halves(dst.shape[0]):
        term = dot(a[rows], b)
        dst[rows, :] = term if minus is None else minus[rows, :] - term


def solve_kernel(
    sizes,
    shots, leaf_inverse, leaf_basis, leaf_back, level_one, level_two, level_three, top_inverse,
    out, w0,
    b, e, p, h, f1, f2, f3, top, a0, g1, g2, g3,
    c0send, c0, c1send, c1, c2send, c2, call,
    z1, z2, z3, w3, w2send, w2, w1send, w1, w0send,
    local_sem, send_sem, recv_sem, z_send, z_recv,
):
    n, rank, nodes = sizes
    lanes1 = b.shape[3]
    lanes2, lanes3 = lanes1 // 2, lanes1 // 4
    me = lax.axis_index("leaf")
    core, x, y, z = me % 2, me // 2 % 2, me // 4 % 2, me // 8
    to_core = me + 1 - 2 * core
    to_x = me + 2 - 4 * x
    to_y = me + 4 - 8 * y
    to_z = {k: me + 8 * (flip_of(z, k) - z) for k in range(1, nodes)}
    inner = (z % 4 == 1) | (z % 4 == 2)
    def ds(index, size):
        return pl.ds(pl.multiple_of(index * size, size), size)

    count = [0]
    local = {}

    def load(name, src, dst):
        local[name] = pltpu.make_async_copy(src, dst, local_sem.at[len(local)])
        local[name].start()

    remote = {}

    def send(name, src, dst, to):
        prepare(name, src, dst, to)
        remote[name].start()

    def prepare(name, src, dst, to):
        i = len(remote)
        remote[name] = pltpu.make_async_remote_copy(
            src_ref=src, dst_ref=dst, send_sem=send_sem.at[i], recv_sem=recv_sem.at[i],
            device_id=(to,), device_id_type=MESH,
        )

    def arrived(name):
        remote[name].wait_recv()

    def columns(c, side):
        half = core if side == 0 else 1 - core
        return ds(c * 2 + half, lanes1)

    load("p", leaf_basis, p)
    load("e", leaf_inverse, e)
    load("b01", shots.at[:, columns(0, 1)], b.at[0, 1])
    load("b00", shots.at[:, columns(0, 0)], b.at[0, 0])
    rows1, rows2, rows3, rows4 = (r.shape[0] for r in (level_one, level_two, level_three, top_inverse))
    slot2, slot3 = x * 2 + core, y * 4 + x * 2 + core
    load("f1", level_one, f1.at[ds(core, rows1)])
    load("b11", shots.at[:, columns(1, 1)], b.at[1, 1])
    load("b10", shots.at[:, columns(1, 0)], b.at[1, 0])
    load("f2", level_two, f2.at[ds(slot2, rows2)])
    load("f3", level_three, f3.at[ds(slot3, rows3)])
    load("top", top_inverse, top.at[ds(slot3, rows4)])
    load("h", leaf_back, h)

    barrier = pltpu.get_barrier_semaphore()

    def between(k):
        return inner if k == 3 else None

    def guarded(condition, action):
        action() if condition is None else pl.when(condition)(action)

    def greet(peer):
        pl.semaphore_signal(barrier, inc=1, device_id=(peer,), device_id_type=MESH)

    for peer in (to_core, to_x, to_y):
        greet(peer)
    for k, peer in to_z.items():
        guarded(between(k), functools.partial(greet, peer))
    far = 1 - inner.astype(jnp.int32) if nodes > 3 else 0
    pl.semaphore_wait(barrier, 3 + len(to_z) - far)

    kq, fc = pl.ds(0, 3 * rank), pl.ds(3 * rank, rank)
    slot2x = (1 - x) * 2 + core
    slot3x, slot3y = y * 4 + (1 - x) * 2 + core, (1 - y) * 4 + x * 2 + core
    slot3xy = (1 - y) * 4 + (1 - x) * 2 + core
    send("f1", level_one, f1.at[ds(core, rows1)], to_core)
    send("f3y", level_three.at[:, kq], f3.at[ds(slot3, rows3), kq], to_y)
    send("f3x", level_three.at[:, kq], f3.at[ds(slot3, rows3), kq], to_x)
    send("f2x", level_two.at[:, kq], f2.at[ds(slot2, rows2), kq], to_x)
    send("f2c", level_two, f2.at[ds(slot2, rows2)], to_core)
    send("f3c", level_three, f3.at[ds(slot3, rows3)], to_core)
    send("tc", top_inverse, top.at[ds(slot3, rows4)], to_core)

    def forward(name, buf, slot, rows, cols, to):
        view = buf.at[ds(slot, rows), cols]
        send(name, view, view, to)

    cols4 = pl.ds(0, top.shape[1])
    share = ((top, rows4, cols4), (f3, rows3, fc))
    for name, (buf, rows, cols) in zip(("t", "f"), share):
        src = top_inverse if name == "t" else level_three.at[:, fc]
        prepare(name + "x", src, buf.at[ds(slot3, rows), cols], to_x)
        view = buf.at[ds(slot3x, rows), cols]
        prepare(name + "xy", view, view, to_y)
        prepare(name + "xc", view, view, to_core)

    def forward_late(names):
        for name in names:
            remote[name + "x"].wait_recv()
            remote[name + "xy"].start()
            remote[name + "xc"].start()

    for name, buf, slot, rows in (("f3xy", f3, slot3xy, rows3), ("f2x", f2, slot2x, rows2)):
        view = buf.at[ds(slot, rows), kq]
        prepare(name + "c", view, view, to_core)

    def forward_kq(condition):
        @pl.when(condition)
        def _():
            for key in ("f3xy", "f2x"):
                remote[key].wait_recv()
                remote[key + "c"].start()

    local["p"].wait()
    local["e"].wait()
    a0[...] = dot(p[...], e[...])
    for c in range(CHUNKS):
        local[f"b{c}1"].wait()
        c0send[c] = dot(a0[...], b[c, 1])
        send(f"c0_{c}", c0send.at[c], c0.at[c, ds(core, rank)], to_core)
        local[f"b{c}0"].wait()
        c0[c, ds(core, rank), :] = dot(a0[...], b[c, 0])

    def pieces(first, last):
        def piece(i, carry):
            i, part = i // DEPTHS, i % DEPTHS
            rows = pl.ds(pl.multiple_of(i % 2 * half_leaf, half_leaf), half_leaf)
            depth = ds(part, e.shape[1] // DEPTHS)
            c, side = i // 4, i // 2 % 2
            total = jnp.where(part == 0, 0.0, out[c, side, rows, :])
            out[c, side, rows, :] = total + dot(e[rows, depth], b[c, side, depth, :])
            return carry

        lax.fori_loop(first, last, piece, 0)

    half_leaf = e.shape[0] // 2

    def z1_piece(c):
        z1[c] = dot(f1[:, : 2 * rank], c0[c])

    local["f1"].wait()
    arrived("f1")
    g1[...] = dot_t(f1[:, 2 * rank : 3 * rank], f1[:, : 2 * rank])
    pieces(0, 2 * core)
    arrived("f3x")
    forward("f3xy", f3, slot3x, rows3, kq, to_y)
    forward("f3xc", f3, slot3x, rows3, kq, to_core)
    arrived("f3y")
    forward("f3yc", f3, slot3y, rows3, kq, to_core)
    send("ty", top_inverse, top.at[ds(slot3, rows4)], to_y)
    send("f3fy", level_three.at[:, fc], f3.at[ds(slot3, rows3), fc], to_y)
    pieces(2 * core, 7 * core)
    forward_kq(core == 1)
    for c in range(CHUNKS):
        arrived(f"c0_{c}")
        product(c1send.at[c], g1, c0[c, :, ds(1 - x, lanes2)])
        for part, half in enumerate((1 - y, y)):
            cols = ds(half, lanes3)
            if (c, part) == (CHUNKS - 1, 1):
                remote["tx"].start()
                remote["fx"].start()
            send(f"c1_{c}{part}", c1send.at[c, :, cols], c1.at[c, ds(x, rank), cols], to_x)
        product(c1.at[c, ds(x, rank)], g1, c0[c, :, ds(x, lanes2)])
    send("f2fx", level_two.at[:, fc], f2.at[ds(slot2, rows2), fc], to_x)

    def up_two(c, part):
        arrived(f"c1_{c}{part}")
        if part == 0:
            cols = ds(1 - y, lanes3)
            product(c2send.at[c], g2, c1[c, :, cols])
            send(f"c2_{c}", c2send.at[c], c2.at[c, ds(y, rank)], to_y)
        else:
            product(c2.at[c, ds(y, rank)], g2, c1[c, :, ds(y, lanes3)])

    def up_three(c):
        arrived(f"c2_{c}")
        product(call.at[c, ds(z, rank)], g3, c2[c])
        for k in sorted(to_z, key=lambda k: (k != 2, -k)):
            guarded(between(k), block(c, k).start)

    def block(c, k):
        view = call.at[c, ds(z, rank)]
        i = c * nodes + k
        return pltpu.make_async_remote_copy(
            src_ref=view, dst_ref=view, send_sem=z_send.at[i], recv_sem=z_recv.at[i],
            device_id=(to_z[k],), device_id_type=MESH,
        )

    def passed(c):
        view = call.at[c, ds(flip_of(z, 2), rank)]
        return pltpu.make_async_remote_copy(
            src_ref=view, dst_ref=view, send_sem=z_send.at[c * nodes], recv_sem=z_recv.at[c * nodes + 3],
            device_id=(to_z[1],), device_id_type=MESH,
        )

    def pass_on(c):
        if nodes > 3:
            @pl.when(inner)
            def _():
                block(c, 2).wait_recv()
                passed(c).start()

    def gathered(c):
        for k in to_z:
            guarded(~inner if k == 2 and nodes > 3 else None, block(c, k).wait_recv)

    pieces(7 * core, 6 + core)
    forward_kq(core == 0)
    local["f2"].wait()
    arrived("f2c")
    arrived("f2xc")
    g2[...] = dot_t(f2[:, 2 * rank : 3 * rank], f2[:, : 2 * rank])
    pieces(7 * core, 9 * core)
    up_two(0, 0)
    local["f3"].wait()
    for name in ("f3c", "f3yc", "f3xc", "f3xyc"):
        arrived(name)
    g3[...] = dot_t(f3[:, 2 * rank : 3 * rank], f3[:, : 2 * rank])
    z1_piece(0)
    up_two(0, 1)
    product(z2.at[0], f2.at[:, : 2 * rank], c1[0])
    arrived("ty")
    forward("tyc", top, slot3y, rows4, cols4, to_core)
    arrived("f3fy")
    forward("f3fyc", f3, slot3y, rows3, fc, to_core)
    pieces(6 + 3 * core, 7 + 2 * core)
    up_three(0)
    product(z3.at[0], f3.at[:, : 2 * rank], c2[0])
    up_two(1, 0)
    z1_piece(1)
    pieces(7 + 2 * core, 9 + core)
    forward_late("tf")
    up_two(1, 1)
    pass_on(0)
    up_three(1)
    product(z3.at[1], f3.at[:, : 2 * rank], c2[1])
    product(z2.at[1], f2.at[:, : 2 * rank], c1[1])
    pieces(9 + core, 11 - core)
    arrived("txy")
    forward("txyc", top, slot3xy, rows4, cols4, to_core)
    arrived("fxy")
    forward("fxyc", f3, slot3xy, rows3, fc, to_core)
    arrived("f2fx")
    forward("f2fxc", f2, slot2x, rows2, fc, to_core)
    local["top"].wait()
    for name in ("tc", "tyc", "txc", "txyc", "f3fyc", "fxc", "fxyc"):
        arrived(name)

    def down_three(c):
        gathered(c)
        product(w3, top, call[c])
        other = pl.ds(pl.multiple_of((1 - y) * rank, rank), rank)
        own = pl.ds(pl.multiple_of(y * rank, rank), rank)
        product(w2send.at[c], f3.at[other, 3 * rank :], w3[...], z3.at[c, other])
        send(f"w2_{c}", w2send.at[c], w2.at[c, :, ds(y, lanes3)], to_y)
        product(w2.at[c, :, ds(y, lanes3)], f3.at[own, 3 * rank :], w3[...], z3.at[c, own])

    def down_two(c, part):
        half = y if part == 0 else 1 - y
        if part == 1:
            arrived(f"w2_{c}")
        cols = ds(half, lanes3)
        lanes = pl.ds(pl.multiple_of(x * lanes2 + half * lanes3, lanes3), lanes3)
        other = pl.ds(pl.multiple_of((1 - x) * rank, rank), rank)
        own = pl.ds(pl.multiple_of(x * rank, rank), rank)
        product(w1send.at[c, :, cols], f2.at[other, 3 * rank :], w2[c, :, cols], z2.at[c, other, cols])
        send(f"w1_{c}{part}", w1send.at[c, :, cols], w1.at[c, :, lanes], to_x)
        product(w1.at[c, :, lanes], f2.at[own, 3 * rank :], w2[c, :, cols], z2.at[c, own, cols])

    def down_one(c, part):
        half = x if part == 0 else 1 - x
        if part == 1:
            arrived(f"w1_{c}0")
            arrived(f"w1_{c}1")
        lanes = ds(half, lanes2)
        other = pl.ds(pl.multiple_of((1 - core) * rank, rank), rank)
        own = pl.ds(pl.multiple_of(core * rank, rank), rank)
        product(w0send.at[c, :, lanes], f1.at[other, 3 * rank :], w1[c, :, lanes], z1.at[c, other, lanes])
        send(f"w0_{c}{part}", w0send.at[c, :, lanes], w0.at[c, 1, :, lanes], to_core)
        product(w0.at[c, 0, :, lanes], f1.at[own, 3 * rank :], w1[c, :, lanes], z1.at[c, own, lanes])

    def last(c, side, half):
        lanes = ds(half, lanes2)
        product(out.at[c, side, :, lanes], h, w0[c, side, :, lanes], out.at[c, side, :, lanes])

    pieces(11 - core, 11 + core)
    down_three(0)
    arrived("f2fxc")
    down_two(0, 0)
    pass_on(1)
    pieces(11 + core, 13 + core)
    down_two(0, 1)
    down_one(0, 0)
    down_three(1)
    down_two(1, 0)
    pieces(13 + core, 16)
    down_one(0, 1)
    local["h"].wait()
    down_two(1, 1)
    down_one(1, 0)
    out[0, 0] = out[0, 0] - dot(h[...], w0[0, 0])
    last(1, 0, x)
    arrived("w0_00")
    arrived("w0_01")
    out[0, 1] = out[0, 1] - dot(h[...], w0[0, 1])
    arrived("w0_10")
    last(1, 1, x)
    down_one(1, 1)
    last(1, 0, 1 - x)
    arrived("w0_11")
    for copy in remote.values():
        copy.wait_send()
    for c in range(CHUNKS):
        for k in to_z:
            guarded(between(k), block(c, k).wait_send)
        if nodes > 3:
            pl.when(inner)(passed(c).wait_send)


def flip_of(value, mask):
    bit = 1
    while bit <= mask:
        if mask & bit:
            value = value + bit - 2 * bit * (value // bit % 2)
        bit *= 2
    return value


def finish_kernel(part, w0, h, out, done, sem):
    me = lax.axis_index("leaf")
    core, x = me % 2, me // 2 % 2
    lanes1 = part.shape[3]
    lanes2 = lanes1 // 2
    copies = []

    def columns(c, side, half):
        start = c * 4 + (core if side == 0 else 1 - core) * 2 + half
        return pl.ds(pl.multiple_of(start * lanes2, lanes2), lanes2)

    def store(src, cols):
        copies.append(pltpu.make_async_copy(src, out.at[:, cols], sem.at[len(copies)]))
        copies[-1].start()

    for c in range(CHUNKS):
        for side in range(2):
            for half in (x, 1 - x):
                lanes = pl.ds(pl.multiple_of(half * lanes2, lanes2), lanes2)
                if len(copies) < 4 * CHUNKS - 1:
                    store(part.at[c, side, :, lanes], columns(c, side, half))
    for rows in halves(done.shape[0]):
        done[rows, :] = part[1, 1, rows, lanes] - dot(h[rows, :], w0[1, 1, :, lanes])
    store(done, columns(c, side, half))
    for copy in copies:
        copy.wait()


def shards(n, *args):
    shots, leaf_inverse, leaf_basis, leaf_back, level_one, level_two, level_three, top_inverse = args
    rank, rows = leaf_basis.shape
    nodes = n // 2**LEVELS
    width = shots.shape[1] // CHUNKS
    l1, l2, l3 = width // 2, width // 4, width // 8
    f32 = jnp.float32
    vmem = lambda *shape: pltpu.VMEM(shape, f32)
    z_count = CHUNKS * nodes
    part, w0 = pl.pallas_call(
        functools.partial(solve_kernel, (n, rank, nodes)),
        name="solve",
        out_shape=(
            pltpu.VMEM((CHUNKS, 2, rows, l1), f32),
            pltpu.VMEM((CHUNKS, 2, rank, l1), f32),
        ),
        in_specs=[pl.BlockSpec(memory_space=pl.ANY)] * 8,
        out_specs=[pl.BlockSpec(memory_space=pltpu.VMEM)] * 2,
        scratch_shapes=[
            vmem(CHUNKS, 2, rows, l1),
            vmem(*leaf_inverse.shape),
            vmem(*leaf_basis.shape),
            vmem(*leaf_back.shape),
            vmem(2 * rank, 4 * rank),
            vmem(2 * rank, 4 * rank),
            vmem(2 * rank, 4 * rank),
            vmem(rank, nodes * rank),
            vmem(rank, rows),
            vmem(rank, 2 * rank),
            vmem(rank, 2 * rank),
            vmem(rank, 2 * rank),
            vmem(CHUNKS, rank, l1),
            vmem(CHUNKS, 2 * rank, l1),
            vmem(CHUNKS, rank, l2),
            vmem(CHUNKS, 2 * rank, l2),
            vmem(CHUNKS, rank, l3),
            vmem(CHUNKS, 2 * rank, l3),
            vmem(CHUNKS, nodes * rank, l3),
            vmem(CHUNKS, 2 * rank, l1),
            vmem(CHUNKS, 2 * rank, l2),
            vmem(CHUNKS, 2 * rank, l3),
            vmem(rank, l3),
            vmem(CHUNKS, rank, l3),
            vmem(CHUNKS, rank, l2),
            vmem(CHUNKS, rank, l2),
            vmem(CHUNKS, rank, l1),
            vmem(CHUNKS, rank, l1),
            pltpu.SemaphoreType.DMA((16,)),
            pltpu.SemaphoreType.DMA((64,)),
            pltpu.SemaphoreType.DMA((64,)),
            pltpu.SemaphoreType.DMA((z_count,)),
            pltpu.SemaphoreType.DMA((z_count,)),
        ],
        compiler_params=pltpu.CompilerParams(
            collective_id=0, has_side_effects=True, vmem_limit_bytes=VMEM_LIMIT
        ),
    )(*args)
    return pl.pallas_call(
        finish_kernel,
        name="finish",
        out_shape=jax.ShapeDtypeStruct(shots.shape, f32),
        in_specs=[pl.BlockSpec(memory_space=pltpu.VMEM)] * 3,
        out_specs=pl.BlockSpec(memory_space=pl.ANY),
        scratch_shapes=[vmem(rows, l2), pltpu.SemaphoreType.DMA((4 * CHUNKS,))],
        compiler_params=pltpu.CompilerParams(vmem_limit_bytes=24 * 2**20),
    )(part, w0, leaf_back)


def solution(mesh):
    return jax.shard_map(
        functools.partial(shards, mesh.shape["leaf"]),
        mesh=mesh,
        in_specs=(P("leaf", None),) * 8,
        out_specs=P("leaf", None),
        check_vma=False,
    )
```

```python
import functools

import jax
import jax.numpy as jnp
from jax import lax
from jax.experimental import pallas as pl
from jax.experimental.pallas import tpu as pltpu
from jax.sharding import PartitionSpec as P

LEVELS = 3
CHUNKS = 2
DEPTHS = 2
LOCALS, REMOTES = 11, 44
HIGH = lax.Precision.HIGH
MESH = pl.DeviceIdType.MESH
VMEM_LIMIT = 48 * 2**20


def dot(a, b):
    return jnp.dot(a, b, precision=HIGH, preferred_element_type=jnp.float32)


def dot_t(a, b):
    dims = (((0,), (0,)), ((), ()))
    return lax.dot_general(a, b, dims, precision=HIGH, preferred_element_type=jnp.float32)


def halves(rows):
    return [pl.ds(i * (rows // 2), rows // 2) for i in range(2)]


def product(dst, a, b, minus=None):
    for rows in halves(dst.shape[0]):
        term = dot(a[rows], b)
        dst[rows, :] = term if minus is None else minus[rows, :] - term


def solve_kernel(
    sizes,
    shots, leaf_inverse, leaf_basis, leaf_back, level_one, level_two, level_three, top_inverse,
    out, w0,
    b, e, p, h, f1, f2, f3, top, a0, g1, g2, g3,
    c0send, c0, c1send, c1, c2send, c2, call,
    z1, z2, z3, w3, w2send, w2, w1send, w1, w0send,
    local_sem, send_sem, recv_sem, z_send, z_recv,
):
    n, rank, nodes = sizes
    lanes1 = b.shape[3]
    lanes2, lanes3 = lanes1 // 2, lanes1 // 4
    me = lax.axis_index("leaf")
    core, x, y, z = me % 2, me // 2 % 2, me // 4 % 2, me // 8
    to_core = me + 1 - 2 * core
    to_x = me + 2 - 4 * x
    to_y = me + 4 - 8 * y
    to_z = {k: me + 8 * (flip_of(z, k) - z) for k in range(1, nodes)}
    inner = (z % 4 == 1) | (z % 4 == 2)
    def ds(index, size):
        return pl.ds(pl.multiple_of(index * size, size), size)

    count = [0]
    local = {}

    def load(name, src, dst):
        local[name] = pltpu.make_async_copy(src, dst, local_sem.at[len(local)])
        local[name].start()

    remote = {}

    def send(name, src, dst, to):
        prepare(name, src, dst, to)
        remote[name].start()

    def prepare(name, src, dst, to):
        i = len(remote)
        remote[name] = pltpu.make_async_remote_copy(
            src_ref=src, dst_ref=dst, send_sem=send_sem.at[i], recv_sem=recv_sem.at[i],
            device_id=(to,), device_id_type=MESH,
        )

    def arrived(name):
        remote[name].wait_recv()

    def columns(c, side):
        half = core if side == 0 else 1 - core
        return ds(c * 2 + half, lanes1)

    barrier = pltpu.get_barrier_semaphore()

    def between(k):
        return inner if k == 3 else None

    def guarded(condition, action):
        action() if condition is None else pl.when(condition)(action)

    def greet(peer):
        pl.semaphore_signal(barrier, inc=1, device_id=(peer,), device_id_type=MESH)

    for peer in (to_core, to_x, to_y):
        greet(peer)
    for k, peer in to_z.items():
        guarded(between(k), functools.partial(greet, peer))
    far = 1 - inner.astype(jnp.int32) if nodes > 3 else 0
    load("p", leaf_basis, p)
    load("e", leaf_inverse, e)
    load("b01", shots.at[:, columns(0, 1)], b.at[0, 1])
    load("b00", shots.at[:, columns(0, 0)], b.at[0, 0])
    rows1, rows2, rows3, rows4 = (r.shape[0] for r in (level_one, level_two, level_three, top_inverse))
    slot2, slot3 = x * 2 + core, y * 4 + x * 2 + core
    load("f1", level_one, f1.at[ds(core, rows1)])
    load("b11", shots.at[:, columns(1, 1)], b.at[1, 1])
    load("b10", shots.at[:, columns(1, 0)], b.at[1, 0])
    load("f2", level_two, f2.at[ds(slot2, rows2)])
    load("f3", level_three, f3.at[ds(slot3, rows3)])
    load("top", top_inverse, top.at[ds(slot3, rows4)])
    load("h", leaf_back, h)

    pl.semaphore_wait(barrier, 3 + len(to_z) - far)

    kq, fc = pl.ds(0, 3 * rank), pl.ds(3 * rank, rank)
    slot2x = (1 - x) * 2 + core
    slot3x, slot3y = y * 4 + (1 - x) * 2 + core, (1 - y) * 4 + x * 2 + core
    slot3xy = (1 - y) * 4 + (1 - x) * 2 + core
    send("f3x", level_three.at[:, kq], f3.at[ds(slot3, rows3), kq], to_x)
    send("f2x", level_two.at[:, kq], f2.at[ds(slot2, rows2), kq], to_x)
    send("f3y", level_three.at[:, kq], f3.at[ds(slot3, rows3), kq], to_y)
    send("f1", level_one, f1.at[ds(core, rows1)], to_core)
    send("f2c", level_two, f2.at[ds(slot2, rows2)], to_core)
    send("f3c", level_three, f3.at[ds(slot3, rows3)], to_core)
    send("tc", top_inverse, top.at[ds(slot3, rows4)], to_core)

    def forward(name, buf, slot, rows, cols, to):
        view = buf.at[ds(slot, rows), cols]
        send(name, view, view, to)

    cols4 = pl.ds(0, top.shape[1])
    share = ((top, rows4, cols4), (f3, rows3, fc))
    for name, (buf, rows, cols) in zip(("t", "f"), share):
        src = top_inverse if name == "t" else level_three.at[:, fc]
        prepare(name + "x", src, buf.at[ds(slot3, rows), cols], to_x)
        view = buf.at[ds(slot3x, rows), cols]
        prepare(name + "xy", view, view, to_y)
        prepare(name + "xc", view, view, to_core)

    def forward_late(names):
        for name in names:
            remote[name + "x"].wait_recv()
            remote[name + "xy"].start()
            remote[name + "xc"].start()

    for name, buf, slot, rows in (("f3xy", f3, slot3xy, rows3), ("f2x", f2, slot2x, rows2)):
        view = buf.at[ds(slot, rows), kq]
        prepare(name + "c", view, view, to_core)

    def forward_kq(condition):
        @pl.when(condition)
        def _():
            for key in ("f3xy", "f2x"):
                remote[key].wait_recv()
                remote[key + "c"].start()

    local["p"].wait()
    local["e"].wait()
    a0[...] = dot(p[...], e[...])
    for c in range(CHUNKS):
        local[f"b{c}1"].wait()
        c0send[c] = dot(a0[...], b[c, 1])
        send(f"c0_{c}", c0send.at[c], c0.at[c, ds(core, rank)], to_core)
        local[f"b{c}0"].wait()
        c0[c, ds(core, rank), :] = dot(a0[...], b[c, 0])

    def pieces(first, last):
        def piece(i, carry):
            i, part = i // DEPTHS, i % DEPTHS
            rows = pl.ds(pl.multiple_of(i % 2 * half_leaf, half_leaf), half_leaf)
            depth = ds(part, e.shape[1] // DEPTHS)
            c, side = i // 4, i // 2 % 2
            total = jnp.where(part == 0, 0.0, out[c, side, rows, :])
            out[c, side, rows, :] = total + dot(e[rows, depth], b[c, side, depth, :])
            return carry

        lax.fori_loop(first, last, piece, 0)

    half_leaf = e.shape[0] // 2

    def z1_piece(c):
        z1[c] = dot(f1[:, : 2 * rank], c0[c])

    local["f1"].wait()
    arrived("f1")
    g1[...] = dot_t(f1[:, 2 * rank : 3 * rank], f1[:, : 2 * rank])
    pieces(0, 2 * core)
    arrived("f3x")
    forward("f3xy", f3, slot3x, rows3, kq, to_y)
    forward("f3xc", f3, slot3x, rows3, kq, to_core)
    arrived("f3y")
    forward("f3yc", f3, slot3y, rows3, kq, to_core)
    send("ty", top_inverse, top.at[ds(slot3, rows4)], to_y)
    send("f3fy", level_three.at[:, fc], f3.at[ds(slot3, rows3), fc], to_y)
    pieces(2 * core, 7 * core)
    forward_kq(core == 1)
    for c in range(CHUNKS):
        arrived(f"c0_{c}")
        product(c1send.at[c], g1, c0[c, :, ds(1 - x, lanes2)])
        for part, half in enumerate((1 - y, y)):
            cols = ds(half, lanes3)
            if (c, part) == (CHUNKS - 1, 1):
                remote["tx"].start()
                remote["fx"].start()
            send(f"c1_{c}{part}", c1send.at[c, :, cols], c1.at[c, ds(x, rank), cols], to_x)
        product(c1.at[c, ds(x, rank)], g1, c0[c, :, ds(x, lanes2)])
    send("f2fx", level_two.at[:, fc], f2.at[ds(slot2, rows2), fc], to_x)

    def up_two(c, part):
        arrived(f"c1_{c}{part}")
        if part == 0:
            cols = ds(1 - y, lanes3)
            product(c2send.at[c], g2, c1[c, :, cols])
            send(f"c2_{c}", c2send.at[c], c2.at[c, ds(y, rank)], to_y)
        else:
            product(c2.at[c, ds(y, rank)], g2, c1[c, :, ds(y, lanes3)])

    def up_three(c):
        arrived(f"c2_{c}")
        product(call.at[c, ds(z, rank)], g3, c2[c])
        for k in sorted(to_z, key=lambda k: (k != 2, -k)):
            guarded(between(k), block(c, k).start)

    def block(c, k):
        view = call.at[c, ds(z, rank)]
        i = c * nodes + k
        return pltpu.make_async_remote_copy(
            src_ref=view, dst_ref=view, send_sem=z_send.at[i], recv_sem=z_recv.at[i],
            device_id=(to_z[k],), device_id_type=MESH,
        )

    def passed(c):
        view = call.at[c, ds(flip_of(z, 2), rank)]
        return pltpu.make_async_remote_copy(
            src_ref=view, dst_ref=view, send_sem=z_send.at[c * nodes], recv_sem=z_recv.at[c * nodes + 3],
            device_id=(to_z[1],), device_id_type=MESH,
        )

    def pass_on(c):
        if nodes > 3:
            @pl.when(inner)
            def _():
                block(c, 2).wait_recv()
                passed(c).start()

    def gathered(c):
        for k in to_z:
            guarded(~inner if k == 2 and nodes > 3 else None, block(c, k).wait_recv)

    pieces(7 * core, 6 + core)
    forward_kq(core == 0)
    local["f2"].wait()
    arrived("f2c")
    arrived("f2xc")
    g2[...] = dot_t(f2[:, 2 * rank : 3 * rank], f2[:, : 2 * rank])
    pieces(7 * core, 9 * core)
    up_two(0, 0)
    local["f3"].wait()
    for name in ("f3c", "f3yc", "f3xc", "f3xyc"):
        arrived(name)
    g3[...] = dot_t(f3[:, 2 * rank : 3 * rank], f3[:, : 2 * rank])
    z1_piece(0)
    up_two(0, 1)
    product(z2.at[0], f2.at[:, : 2 * rank], c1[0])
    arrived("ty")
    forward("tyc", top, slot3y, rows4, cols4, to_core)
    arrived("f3fy")
    forward("f3fyc", f3, slot3y, rows3, fc, to_core)
    pieces(6 + 3 * core, 7 + 2 * core)
    up_three(0)
    product(z3.at[0], f3.at[:, : 2 * rank], c2[0])
    up_two(1, 0)
    z1_piece(1)
    pieces(7 + 2 * core, 9 + core)
    forward_late("tf")
    up_two(1, 1)
    pass_on(0)
    up_three(1)
    product(z3.at[1], f3.at[:, : 2 * rank], c2[1])
    product(z2.at[1], f2.at[:, : 2 * rank], c1[1])
    pieces(9 + core, 11 - core)
    arrived("txy")
    forward("txyc", top, slot3xy, rows4, cols4, to_core)
    arrived("fxy")
    forward("fxyc", f3, slot3xy, rows3, fc, to_core)
    arrived("f2fx")
    forward("f2fxc", f2, slot2x, rows2, fc, to_core)
    local["top"].wait()
    for name in ("tc", "tyc", "txc", "txyc", "f3fyc", "fxc", "fxyc"):
        arrived(name)

    def down_three(c):
        gathered(c)
        product(w3, top, call[c])
        other = pl.ds(pl.multiple_of((1 - y) * rank, rank), rank)
        own = pl.ds(pl.multiple_of(y * rank, rank), rank)
        product(w2send.at[c], f3.at[other, 3 * rank :], w3[...], z3.at[c, other])
        send(f"w2_{c}", w2send.at[c], w2.at[c, :, ds(y, lanes3)], to_y)
        product(w2.at[c, :, ds(y, lanes3)], f3.at[own, 3 * rank :], w3[...], z3.at[c, own])

    def down_two(c, part):
        half = y if part == 0 else 1 - y
        if part == 1:
            arrived(f"w2_{c}")
        cols = ds(half, lanes3)
        lanes = pl.ds(pl.multiple_of(x * lanes2 + half * lanes3, lanes3), lanes3)
        other = pl.ds(pl.multiple_of((1 - x) * rank, rank), rank)
        own = pl.ds(pl.multiple_of(x * rank, rank), rank)
        product(w1send.at[c, :, cols], f2.at[other, 3 * rank :], w2[c, :, cols], z2.at[c, other, cols])
        send(f"w1_{c}{part}", w1send.at[c, :, cols], w1.at[c, :, lanes], to_x)
        product(w1.at[c, :, lanes], f2.at[own, 3 * rank :], w2[c, :, cols], z2.at[c, own, cols])

    def down_one(c, part):
        half = x if part == 0 else 1 - x
        if part == 1:
            arrived(f"w1_{c}0")
            arrived(f"w1_{c}1")
        lanes = ds(half, lanes2)
        other = pl.ds(pl.multiple_of((1 - core) * rank, rank), rank)
        own = pl.ds(pl.multiple_of(core * rank, rank), rank)
        product(w0send.at[c, :, lanes], f1.at[other, 3 * rank :], w1[c, :, lanes], z1.at[c, other, lanes])
        send(f"w0_{c}{part}", w0send.at[c, :, lanes], w0.at[c, 1, :, lanes], to_core)
        product(w0.at[c, 0, :, lanes], f1.at[own, 3 * rank :], w1[c, :, lanes], z1.at[c, own, lanes])

    def drain(chosen):
        for name, copy in remote.items():
            if chosen(name):
                copy.wait_send()

    def drain_nodes():
        for c in range(CHUNKS):
            for k in to_z:
                guarded(between(k), block(c, k).wait_send)
            if nodes > 3:
                pl.when(inner)(passed(c).wait_send)

    def last(c, side, half):
        lanes = ds(half, lanes2)
        product(out.at[c, side, :, lanes], h, w0[c, side, :, lanes], out.at[c, side, :, lanes])

    pieces(11 - core, 11 + core)
    down_three(0)
    arrived("f2fxc")
    down_two(0, 0)
    pass_on(1)
    pieces(11 + core, 13 + core)
    drain(lambda name: name[0] != "w")
    down_two(0, 1)
    down_one(0, 0)
    down_three(1)
    down_two(1, 0)
    pieces(13 + core, 16)
    drain_nodes()
    down_one(0, 1)
    local["h"].wait()
    down_two(1, 1)
    down_one(1, 0)
    out[0, 0] = out[0, 0] - dot(h[...], w0[0, 0])
    last(1, 0, x)
    arrived("w0_00")
    arrived("w0_01")
    out[0, 1] = out[0, 1] - dot(h[...], w0[0, 1])
    arrived("w0_10")
    last(1, 1, x)
    down_one(1, 1)
    last(1, 0, 1 - x)
    arrived("w0_11")
    drain(lambda name: name[0] == "w")
    assert (len(local), len(remote)) == (LOCALS, REMOTES)


def flip_of(value, mask):
    bit = 1
    while bit <= mask:
        if mask & bit:
            value = value + bit - 2 * bit * (value // bit % 2)
        bit *= 2
    return value


def finish_kernel(part, w0, h, out, done, sem):
    me = lax.axis_index("leaf")
    core, x = me % 2, me // 2 % 2
    lanes1 = part.shape[3]
    lanes2 = lanes1 // 2
    copies = []

    def columns(c, side, half):
        start = c * 4 + (core if side == 0 else 1 - core) * 2 + half
        return pl.ds(pl.multiple_of(start * lanes2, lanes2), lanes2)

    def store(src, cols):
        copies.append(pltpu.make_async_copy(src, out.at[:, cols], sem.at[len(copies)]))
        copies[-1].start()

    for c in range(CHUNKS):
        for side in range(2):
            for half in (x, 1 - x):
                lanes = pl.ds(pl.multiple_of(half * lanes2, lanes2), lanes2)
                if len(copies) < 4 * CHUNKS - 1:
                    store(part.at[c, side, :, lanes], columns(c, side, half))
    for rows in halves(done.shape[0]):
        done[rows, :] = part[1, 1, rows, lanes] - dot(h[rows, :], w0[1, 1, :, lanes])
    store(done, columns(c, side, half))
    for copy in copies:
        copy.wait()


def shards(n, *args):
    shots, leaf_inverse, leaf_basis, leaf_back, level_one, level_two, level_three, top_inverse = args
    rank, rows = leaf_basis.shape
    nodes = n // 2**LEVELS
    width = shots.shape[1] // CHUNKS
    l1, l2, l3 = width // 2, width // 4, width // 8
    f32 = jnp.float32
    vmem = lambda *shape: pltpu.VMEM(shape, f32)
    z_count = CHUNKS * nodes
    part, w0 = pl.pallas_call(
        functools.partial(solve_kernel, (n, rank, nodes)),
        name="solve",
        out_shape=(
            pltpu.VMEM((CHUNKS, 2, rows, l1), f32),
            pltpu.VMEM((CHUNKS, 2, rank, l1), f32),
        ),
        in_specs=[pl.BlockSpec(memory_space=pl.ANY)] * 8,
        out_specs=[pl.BlockSpec(memory_space=pltpu.VMEM)] * 2,
        scratch_shapes=[
            vmem(CHUNKS, 2, rows, l1),
            vmem(*leaf_inverse.shape),
            vmem(*leaf_basis.shape),
            vmem(*leaf_back.shape),
            vmem(2 * rank, 4 * rank),
            vmem(2 * rank, 4 * rank),
            vmem(2 * rank, 4 * rank),
            vmem(rank, nodes * rank),
            vmem(rank, rows),
            vmem(rank, 2 * rank),
            vmem(rank, 2 * rank),
            vmem(rank, 2 * rank),
            vmem(CHUNKS, rank, l1),
            vmem(CHUNKS, 2 * rank, l1),
            vmem(CHUNKS, rank, l2),
            vmem(CHUNKS, 2 * rank, l2),
            vmem(CHUNKS, rank, l3),
            vmem(CHUNKS, 2 * rank, l3),
            vmem(CHUNKS, nodes * rank, l3),
            vmem(CHUNKS, 2 * rank, l1),
            vmem(CHUNKS, 2 * rank, l2),
            vmem(CHUNKS, 2 * rank, l3),
            vmem(rank, l3),
            vmem(CHUNKS, rank, l3),
            vmem(CHUNKS, rank, l2),
            vmem(CHUNKS, rank, l2),
            vmem(CHUNKS, rank, l1),
            vmem(CHUNKS, rank, l1),
            pltpu.SemaphoreType.DMA((LOCALS,)),
            pltpu.SemaphoreType.DMA((REMOTES,)),
            pltpu.SemaphoreType.DMA((REMOTES,)),
            pltpu.SemaphoreType.DMA((z_count,)),
            pltpu.SemaphoreType.DMA((z_count,)),
        ],
        compiler_params=pltpu.CompilerParams(
            collective_id=0, has_side_effects=True, vmem_limit_bytes=VMEM_LIMIT
        ),
    )(*args)
    return pl.pallas_call(
        finish_kernel,
        name="finish",
        out_shape=jax.ShapeDtypeStruct(shots.shape, f32),
        in_specs=[pl.BlockSpec(memory_space=pltpu.VMEM)] * 3,
        out_specs=pl.BlockSpec(memory_space=pl.ANY),
        scratch_shapes=[vmem(rows, l2), pltpu.SemaphoreType.DMA((4 * CHUNKS,))],
        compiler_params=pltpu.CompilerParams(vmem_limit_bytes=24 * 2**20),
    )(part, w0, leaf_back)


def solution(mesh):
    return jax.shard_map(
        functools.partial(shards, mesh.shape["leaf"]),
        mesh=mesh,
        in_specs=(P("leaf", None),) * 8,
        out_specs=P("leaf", None),
        check_vma=False,
    )
```
